32 devices in a mesh: dp: 8 (over z, y), group: 4 (over x, core).
Axes of the slice: x: 2, y: 2, z: 4, core: 2. Of those that a mesh axis runs over, the one named last changes fastest.
Arguments:
- rewards: bfloat16 [8192, 4096], P(('dp', 'group')), may hold values from -6 to 6
- values: bfloat16 [8192, 4096], P(('dp', 'group')), may hold values from -6 to 6
- lengths: int32 [8192], P(('dp', 'group')), may hold values from 1 to 4096
- decay_rate: float32 [8192], P(('dp', 'group')), may hold values from 3.8146973e-06 to 0.03125
- piece_dest: int32 [8, 8], P('dp'), may hold values from 0 to 7, each once within a row
- row_perm: int32 [64, 128], P(('dp', 'group')), may hold values from 0 to 127, each once within a row
- minibatch: int32 [8192], P(('dp', 'group')), may hold values from 0 to 63
Outputs:
- white_rewards: bfloat16 [8192, 4096], P(('dp', 'group'))
- white_advantage: bfloat16 [8192, 4096], P(('dp', 'group'))
The draws below stay inside these ranges and needn't reach their ends.
Inputs may be any that keep to these rules, and one draw needn't show every extreme that they name: Each row of piece_dest names every index of dp once. Each row of row_perm names every number below 128 once.
All inputs are finite; a program needn't handle non-finite values.
Results may differ from the reference program's by a relative error of at most 0.0049.
Values may be sent and summed in bfloat16 or wider, within the bound.
A program may use at most 64 MiB of HBM per device.

```python
import math
import jax
import jax.numpy as jnp
from jax import lax

LEN = 4096
BLK = 128
ROWS_DEV = 256
MINIBATCHES = 64
ROWS = 8192
BLOCKS = 64
N_DP = 8
N_GROUP = 4


def plant(result, rng, least, high):
    shape = result.shape
    index_at = [jax.random.randint(jax.random.fold_in(rng, axis), (), 0, shape[axis]) for axis in range(len(shape))]
    result = result.at[tuple(index_at)].set(least)
    longest = shape.index(max(shape))
    index_at[longest] = (index_at[longest] + 1) % shape[longest]
    return result.at[tuple(index_at)].set(high)


def shard_levels(rng, dims, pieces, least, high):
    gain, own = 1.0, jax.random.fold_in(rng, 6)
    for dim, blocks in pieces:
        heights = jnp.exp(jax.random.uniform(jax.random.fold_in(own, dim), (blocks,), jnp.float32, least / len(pieces), high / len(pieces)))
        gain = gain * jnp.repeat(heights, dims[dim] // blocks).reshape([-1 if axis == dim else 1 for axis in range(len(dims))])
    return gain


def centred(key, extent, scale, most, pieces=(), kind=jnp.bfloat16):
    entries = scale * jax.random.normal(key, extent, jnp.float32)
    if pieces:
        entries = entries * shard_levels(key, extent, pieces, -0.22, 0.18)
    return jnp.clip(entries, -most, most).astype(kind)


def setup_inputs(seed: int = 0) -> dict:
    streams_of = jax.random.split(jax.random.key(seed), 8)
    return {
        "rewards": centred(streams_of[0], (ROWS, LEN), 1.0, 6.0, ((0, 32),)),
        "values": centred(streams_of[1], (ROWS, LEN), 1.0, 6.0, ((0, 32),)),
        "lengths": plant(jax.random.randint(streams_of[2], (ROWS,), 1, LEN + 1), jax.random.fold_in(streams_of[2], 1), 1, LEN).astype(jnp.int32),
        "decay_rate": jnp.clip(jnp.exp(math.log(0.03125) - 9.010913 * jax.random.uniform(streams_of[3], (ROWS,), jnp.float32) ** shard_levels(streams_of[3], (ROWS,), ((0, 32),), -0.2, 0.2)), 3.814697265625e-06, 0.03125),
        "piece_dest": jax.vmap(lambda own: jax.random.permutation(own, N_DP))(jax.random.split(streams_of[4], N_DP)).reshape((N_DP, N_DP)).astype(jnp.int32),
        "row_perm": jax.vmap(lambda own: jax.random.permutation(own, BLK))(jax.random.split(streams_of[5], BLOCKS)).reshape((BLOCKS, BLK)).astype(jnp.int32),
        "minibatch": plant(jax.random.randint(streams_of[6], (ROWS,), 0, MINIBATCHES), jax.random.fold_in(streams_of[6], 1), 0, MINIBATCHES - 1).astype(jnp.int32),
    }


def reference(rewards, values, lengths, decay_rate, piece_dest, row_perm, minibatch):
    rows_all, span_all = rewards.shape
    position = jnp.arange(span_all, dtype=jnp.int32)
    is_valid = position[None, :] < lengths[:, None]
    next_valid = position[None, :] + 1 < lengths[:, None]
    per_step = jnp.exp(-decay_rate)
    value_f = values.astype(jnp.float32)
    value_next = jnp.concatenate([value_f[:, 1:], jnp.zeros((rows_all, 1), jnp.float32)], axis=1)
    td_error = rewards.astype(jnp.float32) + per_step[:, None] * jnp.where(next_valid, value_next, 0.0) - value_f
    td_error = jnp.where(is_valid, td_error, 0.0)

    def backward(carry, column):
        fresh = column + per_step * carry
        return (fresh, fresh)
    starting = jnp.zeros((rows_all,), jnp.float32)
    final_carry, stacked = lax.scan(backward, starting, td_error.T, reverse=True)
    advantage = stacked.T.astype(jnp.bfloat16)
    piece = ROWS_DEV // N_DP
    source_slot = jnp.argsort(piece_dest, axis=1).astype(jnp.int32)
    out_rows = jnp.arange(rows_all, dtype=jnp.int32)
    device = out_rows // ROWS_DEV
    target = device // N_GROUP
    column_group = device % N_GROUP
    inside = out_rows % ROWS_DEV
    chosen = inside // BLK * BLK + row_perm.reshape(-1).astype(jnp.int32)
    source_dev = chosen // piece
    within = chosen % piece
    source_row = (source_dev * N_GROUP + column_group) * ROWS_DEV + source_slot[source_dev, target] * piece + within
    moved_rewards = jnp.take(rewards, source_row, axis=0).astype(jnp.float32)
    moved_advantage = jnp.take(advantage, source_row, axis=0).astype(jnp.float32)
    moved_lengths = jnp.take(lengths, source_row, axis=0)
    valid = position[None, :] < moved_lengths[:, None]
    moved_rewards = jnp.where(valid, moved_rewards, 0.0)
    moved_advantage = jnp.where(valid, moved_advantage, 0.0)
    count = jax.ops.segment_sum(moved_lengths.astype(jnp.float32), minibatch, num_segments=MINIBATCHES)
    count = jnp.maximum(count, 1.0)

    def whiten(moved):
        mean = jax.ops.segment_sum(lax.optimization_barrier(jnp.sum(moved, axis=1)), minibatch, num_segments=MINIBATCHES) / count
        deviation = jnp.where(valid, moved - mean[minibatch][:, None], 0.0)
        spread = jax.ops.segment_sum(lax.optimization_barrier(jnp.sum(deviation * deviation, axis=1)), minibatch, num_segments=MINIBATCHES) / count
        return (deviation / jnp.sqrt(spread[minibatch][:, None] + 1e-05)).astype(jnp.bfloat16)
    return (whiten(moved_rewards), whiten(moved_advantage))
```

```python
import functools

import jax
import jax.numpy as jnp
from jax import lax
from jax.experimental import pallas as pl
from jax.experimental.pallas import tpu as pltpu
from jax.sharding import PartitionSpec as P

MINIBATCHES = 64


HIGHEST = lax.Precision.HIGHEST


def discounted(rewards, values, lengths, decay_rate):
    rows_here, span = rewards.shape
    block = min(128, span)
    blocks_here = span // block
    position = jnp.arange(span, dtype=jnp.int32)
    is_valid = position[None, :] < lengths[:, None]
    next_valid = position[None, :] + 1 < lengths[:, None]
    per_step = jnp.exp(-decay_rate)
    value_f = values.astype(jnp.float32)
    value_next = jnp.concatenate([value_f[:, 1:], jnp.zeros((rows_here, 1), jnp.float32)], axis=1)
    td_error = (
        rewards.astype(jnp.float32)
        + per_step[:, None] * jnp.where(next_valid, value_next, 0.0)
        - value_f
    )
    td_error = jnp.where(is_valid, td_error, 0.0).reshape(rows_here, blocks_here, block)
    offset = jnp.arange(block, dtype=jnp.float32)
    lower_scale = jnp.exp(-decay_rate[:, None] * offset[None, :])
    upper_scale = jnp.exp(decay_rate[:, None] * offset[None, :])
    triangle = (offset[:, None] >= offset[None, :]).astype(jnp.float32)
    scaled = td_error * lower_scale[:, None, :]
    summed = jnp.einsum("rjk,kt->rjt", scaled, triangle, precision=HIGHEST)
    local_part = summed * upper_scale[:, None, :]
    heads = local_part[:, :, 0]
    block_step = jnp.exp(-decay_rate * block)

    def carry_step(carry, head):
        fresh = head + block_step * carry
        return (fresh, fresh)

    final_carry, starts = lax.scan(carry_step, jnp.zeros_like(decay_rate), heads.T, reverse=True)
    next_heads = jnp.concatenate([starts[1:].T, jnp.zeros((rows_here, 1), jnp.float32)], axis=1)
    reach = jnp.exp(-decay_rate[:, None] * (block - offset[None, :]))
    total = local_part + reach[:, None, :] * next_heads[:, :, None]
    return jnp.where(is_valid, total.reshape(rows_here, span), 0.0).astype(jnp.bfloat16)


def by_target(array, piece_dest):
    peers = piece_dest.shape[1]
    target = piece_dest[0]
    slots = jnp.arange(peers, dtype=jnp.int32)
    source_slot = jnp.sum(jnp.where(target[None, :] == slots[:, None], slots[None, :], 0), axis=1)
    pieces = array.reshape((peers, array.shape[0] // peers) + array.shape[1:])
    return jnp.take(pieces, source_slot, axis=0).reshape(array.shape)


def reorder(received, row_perm):
    blocks_here, block = row_perm.shape
    chooser = (row_perm[:, :, None] == jnp.arange(block, dtype=jnp.int32)[None, None, :]).astype(
        jnp.bfloat16
    )

    def permute_one(member):
        shaped = member.reshape(blocks_here, block, member.shape[-1])
        mixed = jnp.einsum("bim,bmc->bic", chooser, shaped, preferred_element_type=jnp.float32)
        return mixed.astype(jnp.bfloat16).reshape(member.shape)

    return tuple((permute_one(member) for member in received))


def whiten(rewards, advantage, lengths, minibatch):
    rows_here, span = rewards.shape
    position = jnp.arange(span, dtype=jnp.int32)
    is_valid = position[None, :] < lengths[:, None]
    counted = lengths.astype(jnp.float32)
    reward_f = jnp.where(is_valid, rewards.astype(jnp.float32), 0.0)
    advantage_f = jnp.where(is_valid, advantage.astype(jnp.float32), 0.0)
    member = (minibatch[:, None] == jnp.arange(MINIBATCHES, dtype=jnp.int32)[None, :]).astype(
        jnp.float32
    )
    row_terms = jnp.stack(
        [
            counted,
            jnp.sum(reward_f, axis=1),
            jnp.sum(advantage_f, axis=1),
            jnp.sum(reward_f * reward_f, axis=1),
            jnp.sum(advantage_f * advantage_f, axis=1),
        ],
        axis=1,
    )
    totals = lax.psum(jnp.dot(member.T, row_terms, precision=HIGHEST), ("dp", "group"))
    count = jnp.maximum(totals[:, 0], 1.0)
    means = totals[:, 1:3] / count[:, None]
    spreads = totals[:, 3:5] / count[:, None] - means * means
    row_means = jnp.dot(member, means, precision=HIGHEST)
    row_scale = jnp.dot(member, lax.rsqrt(spreads + 1e-05), precision=HIGHEST)
    white_rewards = jnp.where(is_valid, (reward_f - row_means[:, 0:1]) * row_scale[:, 0:1], 0.0)
    white_advantage = jnp.where(
        is_valid, (advantage_f - row_means[:, 1:2]) * row_scale[:, 1:2], 0.0
    )
    return (white_rewards.astype(jnp.bfloat16), white_advantage.astype(jnp.bfloat16))


def plain_local(rewards, values, lengths, decay_rate, piece_dest, row_perm, minibatch):
    blocks_here, block = row_perm.shape
    new_order = (jnp.arange(blocks_here, dtype=jnp.int32)[:, None] * block + row_perm).reshape(-1)
    per_row = jnp.stack([lengths.astype(jnp.float32), decay_rate], axis=1)
    moved_terms = lax.all_to_all(
        by_target(per_row, piece_dest), "dp", split_axis=0, concat_axis=0, tiled=True
    )
    moved_terms = jnp.take(moved_terms, new_order, axis=0)
    lengths_here = moved_terms[:, 0].astype(jnp.int32)
    rate_here = moved_terms[:, 1]
    moved_rewards, moved_second = reorder(
        (
            lax.all_to_all(
                by_target(rewards, piece_dest), "dp", split_axis=0, concat_axis=0, tiled=True
            ),
            lax.all_to_all(
                by_target(values, piece_dest), "dp", split_axis=0, concat_axis=0, tiled=True
            ),
        ),
        row_perm,
    )
    advantage = discounted(moved_rewards, moved_second, lengths_here, rate_here)
    return whiten(moved_rewards, advantage, lengths_here, minibatch)


F32 = jnp.float32
BF16 = jnp.bfloat16
LANES = 128
MESH = pl.DeviceIdType.MESH
NT = (((1,), (1,)), ((), ()))


def exchange_kernel(
    n_dp, n_group,
    rbuf, val_hbm, rate_ref, packed,
    white_r, white_a,
    out_r, out_a, out_st, out_ch,
    vbuf, abuf, rsend, asend, tri, lower, upper, lenb, bstep, carry,
    acc, tbuf, tstage, tsend, trecv, psend, precv, qsend, qrecv, tot,
    load_sem, own_sem, rs_sem, rr_sem, as_sem, ar_sem, ts_sem, tr_sem, ps_sem, pr_sem, qs_sem, qr_sem,
):
    rows, span = rbuf.shape
    blocks = out_ch.shape[0]
    piece = rows // n_dp
    wide = tri.shape[0]
    cuts = ((0, span // 2), (span // 2, 3 * span // 8), (7 * span // 8, span // 8))
    me = lax.axis_index("dp")
    mine = lax.axis_index("group")
    order = sorted(range(1, n_dp), key=lambda d: (abs(2 * d - n_dp), d))

    def dp_peer(d):
        return lax.rem(me + d, n_dp)

    def group_peer(d):
        return lax.rem(mine + d, n_group)

    quarter = rows // 4
    loads = []
    for part in range(4):
        at = pl.ds(part * quarter, quarter)
        loads.append(pltpu.make_async_copy(val_hbm.at[at], vbuf.at[at], load_sem.at[part]))
        loads[-1].start()

    def row_of(kind, b):
        return packed[kind * blocks + b : kind * blocks + b + 1, :].astype(F32)

    barrier = pltpu.get_barrier_semaphore()
    for d in range(1, n_dp):
        pl.semaphore_signal(barrier, inc=1, device_id=(dp_peer(d), mine), device_id_type=MESH)
    for d in range(1, n_group):
        pl.semaphore_signal(barrier, inc=1, device_id=(me, group_peer(d)), device_id_type=MESH)

    targets = [
        jnp.broadcast_to(row_of(3, 0)[:, p : p + 1], (piece, LANES)) for p in range(n_dp)
    ]

    def pick(d, source):
        k = jnp.full((piece, LANES), dp_peer(d), jnp.int32).astype(F32)
        weights = [(target == k).astype(F32).astype(source.dtype) for target in targets]
        for c in range(0, source.shape[1], LANES):
            at = slice(c, c + LANES)
            yield at, sum(source[p * piece : (p + 1) * piece, at] * weights[p] for p in range(n_dp))

    def stage(d, source, target):
        for at, part in pick(d, source):
            target[d, :, at] = part

    stage(order[0], rbuf, rsend)
    pl.semaphore_wait(barrier, n_dp + n_group - 2)

    def remote(src, dst, send, recv, who):
        return pltpu.make_async_remote_copy(
            src_ref=src, dst_ref=dst, send_sem=send, recv_sem=recv,
            device_id=who, device_id_type=MESH,
        )

    sent = []
    second = []
    for d, later in zip(order, order[1:] + [0]):
        stage(later, rbuf, rsend)
        k = dp_peer(d)
        sent.append(remote(rsend.at[d], out_r.at[me], rs_sem.at[d], rr_sem.at[d], (k, mine)))
        sent[-1].start()
    own = [pltpu.make_async_copy(rsend.at[0], out_r.at[me], own_sem.at[0])]
    own[0].start()

    for b in range(blocks):
        at = pl.ds(b * LANES, LANES)
        rate = jnp.transpose(jnp.broadcast_to(rate_ref[b : b + 1, :], (LANES, LANES)))
        length = jnp.transpose(jnp.broadcast_to(row_of(0, b), (LANES, LANES)))
        lenb[at, :] = length.astype(jnp.int32)
        bstep[at, :] = jnp.exp(-rate * wide)
        carry[at, :] = jnp.zeros((LANES, LANES), F32)
        for x in range(4):
            acc[x, at, :] = jnp.zeros((LANES, LANES), F32)
        for h in range(wide // LANES):
            offset = (lax.broadcasted_iota(jnp.int32, (LANES, LANES), 1) + h * LANES).astype(F32)
            lower[at, h * LANES : (h + 1) * LANES] = jnp.exp(-rate * offset)
            upper[at, h * LANES : (h + 1) * LANES] = jnp.exp(rate * offset)
    tri[...] = (
        lax.broadcasted_iota(jnp.int32, (wide, wide), 0)
        >= lax.broadcasted_iota(jnp.int32, (wide, wide), 1)
    ).astype(F32).astype(BF16)
    for load in loads:
        load.wait()

    reps = wide // LANES

    def column_step(i, _):
        col = pl.multiple_of((span // wide - 1 - i) * wide, wide)
        for b in range(blocks):
            at = pl.ds(b * LANES, LANES)
            length = lenb[at, :]
            position = col + lax.broadcasted_iota(jnp.int32, (LANES, wide), 1)
            valid = position < jnp.concatenate([length] * reps, axis=1)
            r = jnp.where(valid, rbuf[at, pl.ds(col, wide)].astype(F32), 0.0)
            s = r * lower[at, :]
            high = s.astype(BF16)
            low = (s - high.astype(F32)).astype(BF16)
            both = jnp.dot(
                jnp.concatenate([high, low], axis=0), tri[...], preferred_element_type=F32
            )
            c = carry[at, :]
            summed = both[:LANES] + both[LANES:] + jnp.concatenate([c] * reps, axis=1)
            carry[at, :] = bstep[at, :] * jnp.broadcast_to(summed[:, :1], (LANES, LANES))
            a = upper[at, :] * summed - vbuf[at, pl.ds(col, wide)].astype(F32)
            a = jnp.where(valid, a, 0.0).astype(BF16)
            abuf[at, pl.ds(col, wide)] = a
            a = a.astype(F32)
            for x, term in enumerate((r, a, r * r, a * a)):
                acc[x, at, :] += sum(term[:, h * LANES : (h + 1) * LANES] for h in range(reps))
        return 0

    lax.fori_loop(0, span // wide, column_step, 0)

    lane = lax.broadcasted_iota(jnp.int32, (LANES, LANES), 1)
    for b in range(blocks):
        at = pl.ds(b * LANES, LANES)
        terms = jnp.where(lane == 0, lenb[at, :].astype(F32), 0.0)
        for x in range(4):
            total = jnp.sum(acc[x, at, :], axis=1, keepdims=True)
            terms = jnp.where(lane == x + 1, total, terms)
        tbuf[at, :] = terms
    tstage[...] = jnp.zeros_like(tstage)

    def stage_second(d, _):
        stage(d, abuf, asend)
        for at, part in pick(d, tbuf):
            tstage[0:piece, :] = part
        tsend[d] = jnp.transpose(tstage[...])[0:8, :]
        return 0

    lax.fori_loop(0, n_dp, stage_second, 0)

    terms_sent = []
    for d in order:
        k = dp_peer(d)
        terms_sent.append(remote(tsend.at[d], trecv.at[me], ts_sem.at[d], tr_sem.at[d], (k, mine)))
        terms_sent[-1].start()
    trecv[me] = tsend[0]

    def send_second(part):
        at = pl.ds(*cuts[part])
        second.append([])
        for d in order:
            k = dp_peer(d)
            second[part].append(
                remote(
                    asend.at[d, :, at], out_a.at[me, :, at],
                    as_sem.at[part, d], ar_sem.at[part, d], (k, mine),
                )
            )
            second[part][-1].start()

    send_second(0)
    own.append(pltpu.make_async_copy(asend.at[0], out_a.at[me], own_sem.at[1]))
    own[1].start()

    for copy in terms_sent:
        copy.wait()

    row = lax.broadcasted_iota(jnp.int32, (LANES, LANES), 0).astype(F32)
    partial = jnp.zeros((8, LANES), F32)
    per_block = LANES // piece
    for b in range(blocks):
        picked = (row == row_of(1, b)).astype(F32)
        member = (row == row_of(2, b)).astype(F32)
        arrived_member = lax.dot_general(
            member.astype(BF16), picked.astype(BF16), NT, preferred_element_type=F32
        )
        terms = trecv[b * per_block]
        for s in range(1, per_block):
            terms = terms + pltpu.roll(trecv[b * per_block + s], s * piece, 1)
        partial = partial + lax.dot_general(
            terms, arrived_member, NT, precision=HIGHEST, preferred_element_type=F32
        )
        out_ch[b] = jnp.transpose(picked).astype(BF16)
        tot[b] = jnp.dot(terms, picked, precision=HIGHEST, preferred_element_type=F32)
    psend[...] = partial
    precv[me] = partial
    sums_sent = []
    for d in order:
        k = dp_peer(d)
        sums_sent.append(remote(psend, precv.at[me], ps_sem.at[d], pr_sem.at[d], (k, mine)))
        sums_sent[-1].start()

    for part in range(1, len(cuts)):
        send_second(part)

    for copy in sums_sent:
        copy.wait()
    partial = precv[0]
    for k in range(1, n_dp):
        partial = partial + precv[k]
    qsend[...] = partial
    qrecv[mine] = partial
    group_sent = []
    for d in range(1, n_group):
        k = group_peer(d)
        group_sent.append(remote(qsend, qrecv.at[mine], qs_sem.at[d], qr_sem.at[d], (me, k)))
        group_sent[-1].start()
    for copy in group_sent:
        copy.wait()
    total = qrecv[0]
    for k in range(1, n_group):
        total = total + qrecv[k]

    count = jnp.maximum(total[0:1, :], 1.0)
    means = total[1:3, :] / count
    spreads = jnp.maximum(total[3:5, :] / count - means * means, 0.0)
    scales = lax.rsqrt(spreads + 1e-05)
    table = jnp.concatenate([means, scales, jnp.zeros((4, LANES), F32)], axis=0)
    for b in range(blocks):
        at = pl.ds(b * LANES, LANES)
        member = (row == row_of(2, b)).astype(F32)
        here = jnp.dot(table, member, precision=HIGHEST, preferred_element_type=F32)
        here = jnp.concatenate(
            [here[0:4, :], tot[b, 0:1, :], jnp.zeros((LANES - 5, LANES), F32)], axis=0
        )
        out_st[at, :] = jnp.transpose(here)

    def whiten_part(x, source, target, start, width):
        tile = min(512, width)

        def tile_step(i, _):
            col = pl.multiple_of(start + i * tile, tile)
            for b in range(blocks):
                at = pl.ds(b * LANES, LANES)
                stats = out_st[at, :]
                position = (col + lax.broadcasted_iota(jnp.int32, (LANES, tile), 1)).astype(F32)
                arrived = source[b * per_block : (b + 1) * per_block, :, pl.ds(col, tile)]
                moved = jnp.dot(
                    out_ch[b], arrived.reshape(LANES, tile), preferred_element_type=F32
                )
                white = (moved - stats[:, x : x + 1]) * stats[:, x + 2 : x + 3]
                white = jnp.where(position < stats[:, 4:5], white, 0.0)
                target[at, pl.ds(col, tile)] = white.astype(BF16)
            return 0

        lax.fori_loop(0, width // tile, tile_step, 0)

    for copy in own + sent:
        copy.wait()
    whiten_part(0, out_r, white_r, 0, span)
    for part, copies in enumerate(second):
        for copy in copies:
            copy.wait_recv()
        whiten_part(1, out_a, white_a, *cuts[part])
    for copies in second:
        for copy in copies:
            copy.wait_send()


def exchange(n_dp, n_group, rewards, values, lengths, decay_rate, piece_dest, row_perm, minibatch):
    rows, span = rewards.shape
    blocks, block = row_perm.shape
    piece = rows // n_dp
    wide = 256
    vmem = pl.BlockSpec(memory_space=pltpu.VMEM)
    far = pl.BlockSpec(memory_space=pltpu.HBM)
    dma = pltpu.SemaphoreType.DMA
    whole = pltpu.VMEM((rows, span), BF16)
    staged = pltpu.VMEM((n_dp, piece, span), BF16)
    factor = pltpu.VMEM((rows, wide), F32)
    column = pltpu.VMEM((rows, LANES), F32)
    small = pltpu.VMEM((n_dp, 8, LANES), F32)
    one = pltpu.VMEM((8, LANES), F32)
    return pl.pallas_call(
        functools.partial(exchange_kernel, n_dp, n_group),
        out_shape=(jax.ShapeDtypeStruct((rows, span), BF16),) * 2,
        in_specs=[vmem, far, vmem, vmem],
        out_specs=(vmem, vmem),
        scratch_shapes=[
            staged, staged, column, pltpu.VMEM((blocks, LANES, LANES), BF16),
            whole, whole, staged, staged,
            pltpu.VMEM((wide, wide), BF16), factor, factor,
            pltpu.VMEM((rows, LANES), jnp.int32), column, column,
            pltpu.VMEM((4, rows, LANES), F32), column, pltpu.VMEM((LANES, LANES), F32),
            small, small, one, small, one, pltpu.VMEM((n_group, 8, LANES), F32),
            pltpu.VMEM((blocks, 8, LANES), F32),
            dma((4,)), dma((2,)), dma((n_dp,)), dma((n_dp,)), dma((3, n_dp)), dma((3, n_dp)),
            dma((n_dp,)), dma((n_dp,)), dma((n_dp,)), dma((n_dp,)), dma((n_group,)), dma((n_group,)),
        ],
        compiler_params=pltpu.CompilerParams(
            collective_id=1, has_side_effects=True, vmem_limit_bytes=50_000_000
        ),
    )(
        rewards, values, decay_rate.reshape(blocks, block),
        jnp.concatenate(
            [
                lengths.reshape(blocks, block),
                row_perm,
                minibatch.reshape(blocks, block),
                jnp.pad(piece_dest, ((0, 0), (0, block - piece_dest.shape[1]))),
            ],
            axis=0,
        ),
    )


def ragged_kernel(
    n_dp, n_group, cap,
    rew_hbm, val_hbm, len_hbm, rate_hbm, dest_hbm, perm_hbm, mini_hbm,
    white_r, white_a, over_out,
    rbuf, vbuf, abuf, len_v, rate_v, perm_v, mini_v, dest_v,
    dsend, psend, dense, packed, chooser, placer, spread,
    out_st, out_ch, tri, lower, upper, lenb, bstep, carry,
    acc, tbuf, tstage, tsend, trecv, psum, precv, qsum, qrecv, tot,
    load_sem, meta_sem, own_sem, ds_sem, dr_sem, ks_sem, kr_sem,
    ts_sem, tr_sem, ps_sem, pr_sem, qs_sem, qr_sem,
):
    rows, span = rbuf.shape
    blocks = out_ch.shape[0]
    piece = rows // n_dp
    half = n_dp // 2
    chunks = span // LANES
    depth = placer.shape[2]
    wide = tri.shape[0]
    cuts = part_cuts(cap)
    me = lax.axis_index("dp")
    mine = lax.axis_index("group")
    side = me // half
    spot = lax.rem(me, half)

    def dp_peer(d):
        return lax.rem(me + d, n_dp)

    def group_peer(d):
        return lax.rem(mine + d, n_group)

    def near(j):
        return side * half + lax.rem(me + j, half)

    def across(j):
        return (1 - side) * half + lax.rem(me + j, half)

    small = []
    for i, (src, dst) in enumerate(
        ((len_hbm, len_v), (dest_hbm, dest_v), (rate_hbm, rate_v), (perm_hbm, perm_v), (mini_hbm, mini_v))
    ):
        small.append(pltpu.make_async_copy(src, dst, meta_sem.at[i]))
        small[-1].start()
    quarter = rows // 4
    loads = []
    for x, (src, dst) in enumerate(((rew_hbm, rbuf), (val_hbm, vbuf))):
        for part in range(4):
            at = pl.ds(part * quarter, quarter)
            loads.append(pltpu.make_async_copy(src.at[at], dst.at[at], load_sem.at[x, part]))
            loads[-1].start()

    barrier = pltpu.get_barrier_semaphore()
    for d in range(1, n_dp):
        pl.semaphore_signal(barrier, inc=1, device_id=(dp_peer(d), mine), device_id_type=MESH)
    for d in range(1, n_group):
        pl.semaphore_signal(barrier, inc=1, device_id=(me, group_peer(d)), device_id_type=MESH)

    lane = lax.broadcasted_iota(jnp.int32, (LANES, LANES), 1)
    sub = lax.broadcasted_iota(jnp.int32, (LANES, LANES), 0)
    before = jnp.logical_and(sub // piece == lane // piece, sub < lane).astype(F32).astype(BF16)
    per_vreg = LANES // piece

    def used(length):
        return ((length + (LANES - 1)) // LANES).astype(F32).astype(BF16)

    for copy in small:
        copy.wait()

    dests = [dest_v[0:1, p : p + 1] for p in range(n_dp)]
    targets = [jnp.broadcast_to(dest.astype(F32), (piece, LANES)) for dest in dests]
    row_dest = []
    for b in range(blocks):
        here = jnp.zeros((16, LANES), jnp.int32)
        for q in range(per_vreg):
            here = jnp.where(lane[0:16] // piece == q, dests[b * per_vreg + q], here)
        row_dest.append(here)
    fold = (sub % piece == lane % piece).astype(F32).astype(BF16)

    def pick(k, source):
        k = jnp.full((piece, LANES), k, jnp.int32).astype(F32)
        weights = [(target == k).astype(F32).astype(source.dtype) for target in targets]
        for c in range(0, source.shape[1], LANES):
            at = slice(c, c + LANES)
            yield at, sum(source[p * piece : (p + 1) * piece, at] * weights[p] for p in range(n_dp))

    def choose(j, over):
        wanted = jnp.zeros((16, LANES), F32)
        for b in range(blocks):
            here = jnp.broadcast_to(len_v[b : b + 1, :], (16, LANES))
            here = jnp.where(row_dest[b] == across(j), here, 0)
            wanted = wanted + jnp.dot(used(here), fold, preferred_element_type=F32)
        base = jnp.dot(wanted.astype(BF16), before, preferred_element_type=F32)
        over = jnp.maximum(over, jnp.where(base + wanted > cap, 1.0, 0.0)[0:8])
        base = base.astype(jnp.int32)[0:1]
        wanted = wanted.astype(jnp.int32)[0:1]
        place = lax.broadcasted_iota(jnp.int32, (cap, LANES), 0)
        for v in range(chunks // per_vreg):
            c = lane[0:1] // piece + v * per_vreg
            key = jnp.where(c < wanted, base + c, -1)
            chooser[j, :, v * LANES : (v + 1) * LANES] = (place == key).astype(F32).astype(BF16)
        return over

    over = lax.fori_loop(0, half, choose, jnp.zeros((8, LANES), F32))

    def pack(x, j, source):
        arranged = jnp.concatenate([part for _, part in pick(across(j), source)], axis=0)
        psend[x, j] = jnp.dot(chooser[j], arranged, preferred_element_type=F32).astype(BF16)

    def copy_dense(x, j, source):
        for at, part in pick(near(j), source):
            dsend[x, j, :, at] = part

    packed_tail = packed.shape[2] - cap
    if packed_tail:
        packed[:, :, cap:, :] = jnp.zeros((2, half, packed_tail, LANES), BF16)

    for load in loads[:4]:
        load.wait()

    def remote(src, dst, send, recv, who):
        return pltpu.make_async_remote_copy(
            src_ref=src, dst_ref=dst, send_sem=send, recv_sem=recv,
            device_id=who, device_id_type=MESH,
        )

    def dense_copy(x, j):
        return remote(
            dsend.at[x, j], dense.at[x, spot], ds_sem.at[x, j], dr_sem.at[x, j], (near(j), mine)
        )

    def packed_copy(x, j, part):
        at = pl.ds(*cuts[x][part])
        return remote(
            psend.at[x, j, at], packed.at[x, spot, at],
            ks_sem.at[x, part, j], kr_sem.at[x, part, j], (across(j), mine),
        )

    order = []
    for j in range(half):
        order.append((0, j))
        if j + 1 < half:
            order.append((1, j + 1))

    def stage(item):
        kind, j = item
        (copy_dense if kind else pack)(0, j, rbuf)

    def issue(x, item):
        kind, j = item
        copy = dense_copy(x, j) if kind else packed_copy(x, j, 0)
        copy.start()
        return copy

    dense_sent = [[], []]
    packed_sent = [[[]], [[] for _ in cuts[1]]]
    stage(order[0])
    pl.semaphore_wait(barrier, n_dp + n_group - 2)
    for item, later in zip(order, order[1:] + [(1, 0)]):
        stage(later)
        (dense_sent[0] if item[0] else packed_sent[0][0]).append(issue(0, item))
    own = [pltpu.make_async_copy(dsend.at[0, 0], dense.at[0, spot], own_sem.at[0])]
    own[0].start()

    for b in range(blocks):
        at = pl.ds(b * LANES, LANES)
        rate = jnp.transpose(jnp.broadcast_to(rate_v[b : b + 1, :], (LANES, LANES)))
        length = jnp.transpose(jnp.broadcast_to(len_v[b : b + 1, :].astype(F32), (LANES, LANES)))
        lenb[at, :] = length.astype(jnp.int32)
        bstep[at, :] = jnp.exp(-rate * wide)
        carry[at, :] = jnp.zeros((LANES, LANES), F32)
        for x in range(4):
            acc[x, at, :] = jnp.zeros((LANES, LANES), F32)
        for i in range(wide // LANES):
            offset = (lane + i * LANES).astype(F32)
            lower[at, i * LANES : (i + 1) * LANES] = jnp.exp(-rate * offset)
            upper[at, i * LANES : (i + 1) * LANES] = jnp.exp(rate * offset)
    tri[...] = (
        lax.broadcasted_iota(jnp.int32, (wide, wide), 0)
        >= lax.broadcasted_iota(jnp.int32, (wide, wide), 1)
    ).astype(F32).astype(BF16)
    for load in loads[4:]:
        load.wait()

    reps = wide // LANES

    def column_step(i, _):
        col = pl.multiple_of((span // wide - 1 - i) * wide, wide)
        for b in range(blocks):
            at = pl.ds(b * LANES, LANES)
            length = lenb[at, :]
            position = col + lax.broadcasted_iota(jnp.int32, (LANES, wide), 1)
            valid = position < jnp.concatenate([length] * reps, axis=1)
            r = jnp.where(valid, rbuf[at, pl.ds(col, wide)].astype(F32), 0.0)
            s = r * lower[at, :]
            high = s.astype(BF16)
            low = (s - high.astype(F32)).astype(BF16)
            both = jnp.dot(
                jnp.concatenate([high, low], axis=0), tri[...], preferred_element_type=F32
            )
            c = carry[at, :]
            summed = both[:LANES] + both[LANES:] + jnp.concatenate([c] * reps, axis=1)
            carry[at, :] = bstep[at, :] * jnp.broadcast_to(summed[:, :1], (LANES, LANES))
            a = upper[at, :] * summed - vbuf[at, pl.ds(col, wide)].astype(F32)
            a = jnp.where(valid, a, 0.0).astype(BF16)
            abuf[at, pl.ds(col, wide)] = a
            a = a.astype(F32)
            for x, term in enumerate((r, a, r * r, a * a)):
                acc[x, at, :] += sum(term[:, i * LANES : (i + 1) * LANES] for i in range(reps))
        return 0

    lax.fori_loop(0, span // wide, column_step, 0)

    for b in range(blocks):
        at = pl.ds(b * LANES, LANES)
        terms = jnp.where(lane == 0, lenb[at, :].astype(F32), 0.0)
        for x in range(4):
            total = jnp.sum(acc[x, at, :], axis=1, keepdims=True)
            terms = jnp.where(lane == x + 1, total, terms)
        tbuf[at, :] = terms
    tstage[...] = jnp.zeros_like(tstage)

    def stage_terms(d, _):
        for at, part in pick(dp_peer(d), tbuf):
            tstage[0:piece, :] = part
        tsend[d] = jnp.transpose(tstage[...])[0:8, :]
        return 0

    lax.fori_loop(0, n_dp, stage_terms, 0)

    def stage_second(j, _):
        copy_dense(1, j, abuf)
        pack(1, j, abuf)
        return 0

    lax.fori_loop(0, half, stage_second, 0)

    terms_sent = []
    for d in range(1, n_dp):
        k = dp_peer(d)
        terms_sent.append(remote(tsend.at[d], trecv.at[me], ts_sem.at[d], tr_sem.at[d], (k, mine)))
        terms_sent[-1].start()
    trecv[me] = tsend[0]

    for item in order:
        (dense_sent[1] if item[0] else packed_sent[1][0]).append(issue(1, item))
    own.append(pltpu.make_async_copy(dsend.at[1, 0], dense.at[1, spot], own_sem.at[1]))
    own[1].start()

    for copy in terms_sent:
        copy.wait()

    row = sub.astype(F32)
    partial = jnp.where(lax.broadcasted_iota(jnp.int32, (8, LANES), 0) == 5, over, 0.0)
    per_block = LANES // piece
    for b in range(blocks):
        picked = (row == perm_v[b : b + 1, :].astype(F32)).astype(F32)
        member = (row == mini_v[b : b + 1, :].astype(F32)).astype(F32)
        arrived_member = lax.dot_general(
            member.astype(BF16), picked.astype(BF16), NT, preferred_element_type=F32
        )
        terms = trecv[b * per_block]
        for s in range(1, per_block):
            terms = terms + pltpu.roll(trecv[b * per_block + s], s * piece, 1)
        partial = partial + lax.dot_general(
            terms, arrived_member, NT, precision=HIGHEST, preferred_element_type=F32
        )
        out_ch[b] = jnp.transpose(picked).astype(BF16)
        tot[b] = jnp.dot(terms, picked, precision=HIGHEST, preferred_element_type=F32)
    psum[...] = partial
    precv[me] = partial
    sums_sent = []
    for d in range(1, n_dp):
        k = dp_peer(d)
        sums_sent.append(remote(psum, precv.at[me], ps_sem.at[d], pr_sem.at[d], (k, mine)))
        sums_sent[-1].start()

    for part in range(1, len(cuts[1])):
        for j in range(half):
            packed_sent[1][part].append(packed_copy(1, j, part))
            packed_sent[1][part][-1].start()

    other = 1 - side
    length = trecv[other * per_block]
    for s in range(1, per_block):
        length = length + pltpu.roll(trecv[other * per_block + s], s * piece, 1)
    length = jnp.broadcast_to(length[0:1], (16, LANES)).astype(jnp.int32)
    wanted = used(length)
    base = jnp.dot(wanted, before, preferred_element_type=F32)
    base = jnp.transpose(jnp.broadcast_to(base[0:1], (LANES, LANES))).astype(jnp.int32)
    wanted = jnp.transpose(jnp.broadcast_to(wanted.astype(F32)[0:1], (LANES, LANES))).astype(jnp.int32)

    def place_chunk(c, _):
        key = jnp.where(c < wanted, base + c, -1)
        at = pl.ds(pl.multiple_of(c * piece, piece), piece)
        for n in range(depth // LANES):
            match = (lane + n * LANES == key).astype(F32).astype(BF16)
            for q in range(half):
                placer[q, at, n * LANES : (n + 1) * LANES] = match[q * piece : (q + 1) * piece]
        return 0

    lax.fori_loop(0, chunks, place_chunk, 0)

    def unpack(x, start, stop, first):
        stop = depth if stop == cap else stop

        def one(q, _):
            got = jnp.dot(
                placer[q, :, start:stop], packed[x, q, start:stop, :], preferred_element_type=F32
            ).astype(BF16)
            at = pl.ds(pl.multiple_of(q * piece, piece), piece)
            for c in range(chunks):
                cols = slice(c * LANES, (c + 1) * LANES)
                part = got[c * piece : (c + 1) * piece]
                spread[x, at, cols] = part if first else spread[x, at, cols] + part
            return 0

        lax.fori_loop(0, half, one, 0)

    for copy in own[:1] + dense_sent[0] + packed_sent[0][0]:
        copy.wait()
    unpack(0, 0, cap, True)

    for copy in sums_sent:
        copy.wait()
    partial = precv[0]
    for k in range(1, n_dp):
        partial = partial + precv[k]
    qsum[...] = partial
    qrecv[mine] = partial
    group_sent = []
    for d in range(1, n_group):
        k = group_peer(d)
        group_sent.append(remote(qsum, qrecv.at[mine], qs_sem.at[d], qr_sem.at[d], (me, k)))
        group_sent[-1].start()
    for copy in group_sent:
        copy.wait()
    total = qrecv[0]
    for k in range(1, n_group):
        total = total + qrecv[k]
    over_out[0] = jnp.max(total[5:6, :])

    count = jnp.maximum(total[0:1, :], 1.0)
    means = total[1:3, :] / count
    spreads = jnp.maximum(total[3:5, :] / count - means * means, 0.0)
    scales = lax.rsqrt(spreads + 1e-05)
    table = jnp.concatenate([means, scales, jnp.zeros((4, LANES), F32)], axis=0)
    for b in range(blocks):
        at = pl.ds(b * LANES, LANES)
        member = (row == mini_v[b : b + 1, :].astype(F32)).astype(F32)
        here = jnp.dot(table, member, precision=HIGHEST, preferred_element_type=F32)
        here = jnp.concatenate(
            [here[0:4, :], tot[b, 0:1, :], jnp.zeros((LANES - 5, LANES), F32)], axis=0
        )
        out_st[at, :] = jnp.transpose(here)

    def whiten_block(x, arrived_at, b, target):
        tile = 512

        def tile_step(i, _):
            col = pl.multiple_of(i * tile, tile)
            at = pl.ds(pl.multiple_of(b * LANES, LANES), LANES)
            stats = out_st[at, :]
            position = (col + lax.broadcasted_iota(jnp.int32, (LANES, tile), 1)).astype(F32)
            moved = jnp.dot(out_ch[b], arrived_at(pl.ds(col, tile)), preferred_element_type=F32)
            white = (moved - stats[:, x : x + 1]) * stats[:, x + 2 : x + 3]
            white = jnp.where(position < stats[:, 4:5], white, 0.0)
            target[at, pl.ds(col, tile)] = white.astype(BF16)
            return 0

        lax.fori_loop(0, span // tile, tile_step, 0)

    def whiten_dense(x, target):
        whiten_block(x, lambda at: dense[x, :, :, at].reshape(LANES, at.size), side, target)

    def whiten_packed(x, target):
        whiten_block(x, lambda at: spread[x, :, at], other, target)

    whiten_dense(0, white_r)
    whiten_packed(0, white_r)
    for copy in own[1:] + dense_sent[1]:
        copy.wait()
    whiten_dense(1, white_a)
    for part, copies in enumerate(packed_sent[1]):
        for copy in copies:
            copy.wait_recv()
        start, size = cuts[1][part]
        unpack(1, start, start + size, part == 0)
    whiten_packed(1, white_a)
    for copies in packed_sent[1]:
        for copy in copies:
            copy.wait_send()


def part_cuts(cap):
    a, b = cap // 256 * 128, cap // 128 * 128
    b = b - 128 if cap - b < 64 else b
    return (((0, cap),), ((0, a), (a, b - a), (b, cap - b)))


def ragged_capacity(rows, n_dp, span):
    chunks = rows // n_dp * (span // LANES)
    return chunks * 23 // 32 // 16 * 16


def ragged(n_dp, n_group, rewards, values, lengths, decay_rate, piece_dest, row_perm, minibatch):
    rows, span = rewards.shape
    blocks, block = row_perm.shape
    piece = rows // n_dp
    half = n_dp // 2
    wide = 256
    cap = ragged_capacity(rows, n_dp, span)
    depth = -(-cap // LANES) * LANES
    chunks = piece * (span // LANES)
    vmem = pl.BlockSpec(memory_space=pltpu.VMEM)
    far = pl.BlockSpec(memory_space=pltpu.HBM)
    dma = pltpu.SemaphoreType.DMA
    whole = pltpu.VMEM((rows, span), BF16)
    factor = pltpu.VMEM((rows, wide), F32)
    column = pltpu.VMEM((rows, LANES), F32)
    small = pltpu.VMEM((n_dp, 8, LANES), F32)
    one = pltpu.VMEM((8, LANES), F32)
    meta = pltpu.VMEM((blocks, LANES), jnp.int32)
    dense = pltpu.VMEM((2, half, piece, span), BF16)
    parts = len(part_cuts(cap)[1])
    return pl.pallas_call(
        functools.partial(ragged_kernel, n_dp, n_group, cap),
        out_shape=(jax.ShapeDtypeStruct((rows, span), BF16),) * 2
        + (jax.ShapeDtypeStruct((1,), F32),),
        in_specs=[far] * 7,
        out_specs=(vmem, vmem, pl.BlockSpec(memory_space=pltpu.SMEM)),
        scratch_shapes=[
            whole, whole, whole, meta, pltpu.VMEM((blocks, LANES), F32), meta, meta,
            pltpu.VMEM((1, n_dp), jnp.int32),
            dense, pltpu.VMEM((2, half, cap, LANES), BF16),
            dense, pltpu.VMEM((2, half, depth, LANES), BF16),
            pltpu.VMEM((half, cap, chunks), BF16), pltpu.VMEM((half, chunks, depth), BF16),
            pltpu.VMEM((2, LANES, span), BF16),
            column, pltpu.VMEM((blocks, LANES, LANES), BF16),
            pltpu.VMEM((wide, wide), BF16), factor, factor,
            pltpu.VMEM((rows, LANES), jnp.int32), column, column,
            pltpu.VMEM((4, rows, LANES), F32), column, pltpu.VMEM((LANES, LANES), F32),
            small, small, one, small, one, pltpu.VMEM((n_group, 8, LANES), F32),
            pltpu.VMEM((blocks, 8, LANES), F32),
            dma((2, 4)), dma((5,)), dma((2,)), dma((2, half)), dma((2, half)),
            dma((2, parts, half)), dma((2, parts, half)),
            dma((n_dp,)), dma((n_dp,)), dma((n_dp,)), dma((n_dp,)), dma((n_group,)), dma((n_group,)),
        ],
        compiler_params=pltpu.CompilerParams(
            collective_id=0, has_side_effects=True, vmem_limit_bytes=60_000_000
        ),
    )(
        rewards, values, lengths.reshape(blocks, block), decay_rate.reshape(blocks, block),
        piece_dest, row_perm, minibatch.reshape(blocks, block),
    )


def local(n_dp, n_group, rewards, values, lengths, decay_rate, piece_dest, row_perm, minibatch):
    rows, span = rewards.shape
    blocks, block = row_perm.shape
    piece = rows // n_dp
    args = (rewards, values, lengths, decay_rate, piece_dest, row_perm, minibatch)
    if piece % 16 or LANES % piece or block != LANES or span % 4096:
        return plain_local(*args)
    whole = functools.partial(exchange, n_dp, n_group)
    if n_dp % 2 or blocks != 2 or n_dp // 2 * piece != LANES:
        return whole(*args)
    white_rewards, white_advantage, over = ragged(n_dp, n_group, *args)
    return lax.cond(
        over[0] > 0.0,
        lambda kept, args: whole(*args),
        lambda kept, args: kept,
        (white_rewards, white_advantage), args,
    )


def solution(mesh):
    return jax.shard_map(
        functools.partial(local, mesh.shape["dp"], mesh.shape["group"]),
        mesh=mesh,
        in_specs=(
            P(("dp", "group"), None),
            P(("dp", "group"), None),
            P(("dp", "group")),
            P(("dp", "group")),
            P("dp", None),
            P(("dp", "group"), None),
            P(("dp", "group")),
        ),
        out_specs=(P(("dp", "group"), None), P(("dp", "group"), None)),
        check_vma=False,
    )
```

```python
import functools

import jax
import jax.numpy as jnp
from jax import lax
from jax.experimental import pallas as pl
from jax.experimental.pallas import tpu as pltpu
from jax.sharding import PartitionSpec as P

MINIBATCHES = 64


HIGHEST = lax.Precision.HIGHEST


def discounted(rewards, values, lengths, decay_rate):
    rows_here, span = rewards.shape
    block = min(128, span)
    blocks_here = span // block
    position = jnp.arange(span, dtype=jnp.int32)
    is_valid = position[None, :] < lengths[:, None]
    next_valid = position[None, :] + 1 < lengths[:, None]
    per_step = jnp.exp(-decay_rate)
    value_f = values.astype(jnp.float32)
    value_next = jnp.concatenate([value_f[:, 1:], jnp.zeros((rows_here, 1), jnp.float32)], axis=1)
    td_error = (
        rewards.astype(jnp.float32)
        + per_step[:, None] * jnp.where(next_valid, value_next, 0.0)
        - value_f
    )
    td_error = jnp.where(is_valid, td_error, 0.0).reshape(rows_here, blocks_here, block)
    offset = jnp.arange(block, dtype=jnp.float32)
    lower_scale = jnp.exp(-decay_rate[:, None] * offset[None, :])
    upper_scale = jnp.exp(decay_rate[:, None] * offset[None, :])
    triangle = (offset[:, None] >= offset[None, :]).astype(jnp.float32)
    scaled = td_error * lower_scale[:, None, :]
    summed = jnp.einsum("rjk,kt->rjt", scaled, triangle, precision=HIGHEST)
    local_part = summed * upper_scale[:, None, :]
    heads = local_part[:, :, 0]
    block_step = jnp.exp(-decay_rate * block)

    def carry_step(carry, head):
        fresh = head + block_step * carry
        return (fresh, fresh)

    final_carry, starts = lax.scan(carry_step, jnp.zeros_like(decay_rate), heads.T, reverse=True)
    next_heads = jnp.concatenate([starts[1:].T, jnp.zeros((rows_here, 1), jnp.float32)], axis=1)
    reach = jnp.exp(-decay_rate[:, None] * (block - offset[None, :]))
    total = local_part + reach[:, None, :] * next_heads[:, :, None]
    return jnp.where(is_valid, total.reshape(rows_here, span), 0.0).astype(jnp.bfloat16)


def by_target(array, piece_dest):
    peers = piece_dest.shape[1]
    target = piece_dest[0]
    slots = jnp.arange(peers, dtype=jnp.int32)
    source_slot = jnp.sum(jnp.where(target[None, :] == slots[:, None], slots[None, :], 0), axis=1)
    pieces = array.reshape((peers, array.shape[0] // peers) + array.shape[1:])
    return jnp.take(pieces, source_slot, axis=0).reshape(array.shape)


def reorder(received, row_perm):
    blocks_here, block = row_perm.shape
    chooser = (row_perm[:, :, None] == jnp.arange(block, dtype=jnp.int32)[None, None, :]).astype(
        jnp.bfloat16
    )

    def permute_one(member):
        shaped = member.reshape(blocks_here, block, member.shape[-1])
        mixed = jnp.einsum("bim,bmc->bic", chooser, shaped, preferred_element_type=jnp.float32)
        return mixed.astype(jnp.bfloat16).reshape(member.shape)

    return tuple((permute_one(member) for member in received))


def whiten(rewards, advantage, lengths, minibatch):
    rows_here, span = rewards.shape
    position = jnp.arange(span, dtype=jnp.int32)
    is_valid = position[None, :] < lengths[:, None]
    counted = lengths.astype(jnp.float32)
    reward_f = jnp.where(is_valid, rewards.astype(jnp.float32), 0.0)
    advantage_f = jnp.where(is_valid, advantage.astype(jnp.float32), 0.0)
    member = (minibatch[:, None] == jnp.arange(MINIBATCHES, dtype=jnp.int32)[None, :]).astype(
        jnp.float32
    )
    row_terms = jnp.stack(
        [
            counted,
            jnp.sum(reward_f, axis=1),
            jnp.sum(advantage_f, axis=1),
            jnp.sum(reward_f * reward_f, axis=1),
            jnp.sum(advantage_f * advantage_f, axis=1),
        ],
        axis=1,
    )
    totals = lax.psum(jnp.dot(member.T, row_terms, precision=HIGHEST), ("dp", "group"))
    count = jnp.maximum(totals[:, 0], 1.0)
    means = totals[:, 1:3] / count[:, None]
    spreads = totals[:, 3:5] / count[:, None] - means * means
    row_means = jnp.dot(member, means, precision=HIGHEST)
    row_scale = jnp.dot(member, lax.rsqrt(spreads + 1e-05), precision=HIGHEST)
    white_rewards = jnp.where(is_valid, (reward_f - row_means[:, 0:1]) * row_scale[:, 0:1], 0.0)
    white_advantage = jnp.where(
        is_valid, (advantage_f - row_means[:, 1:2]) * row_scale[:, 1:2], 0.0
    )
    return (white_rewards.astype(jnp.bfloat16), white_advantage.astype(jnp.bfloat16))


def plain_local(rewards, values, lengths, decay_rate, piece_dest, row_perm, minibatch):
    blocks_here, block = row_perm.shape
    new_order = (jnp.arange(blocks_here, dtype=jnp.int32)[:, None] * block + row_perm).reshape(-1)
    per_row = jnp.stack([lengths.astype(jnp.float32), decay_rate], axis=1)
    moved_terms = lax.all_to_all(
        by_target(per_row, piece_dest), "dp", split_axis=0, concat_axis=0, tiled=True
    )
    moved_terms = jnp.take(moved_terms, new_order, axis=0)
    lengths_here = moved_terms[:, 0].astype(jnp.int32)
    rate_here = moved_terms[:, 1]
    moved_rewards, moved_second = reorder(
        (
            lax.all_to_all(
                by_target(rewards, piece_dest), "dp", split_axis=0, concat_axis=0, tiled=True
            ),
            lax.all_to_all(
                by_target(values, piece_dest), "dp", split_axis=0, concat_axis=0, tiled=True
            ),
        ),
        row_perm,
    )
    advantage = discounted(moved_rewards, moved_second, lengths_here, rate_here)
    return whiten(moved_rewards, advantage, lengths_here, minibatch)


F32 = jnp.float32
BF16 = jnp.bfloat16
LANES = 128
MESH = pl.DeviceIdType.MESH
NT = (((1,), (1,)), ((), ()))


def exchange_kernel(
    n_dp, n_group,
    rbuf, val_hbm, rate_ref, packed,
    white_r, white_a,
    out_r, out_a, out_st, out_ch,
    vbuf, abuf, rsend, asend, tri, lower, upper, lenb, bstep, carry,
    acc, tbuf, tstage, tsend, trecv, psend, precv, qsend, qrecv, tot,
    load_sem, own_sem, rs_sem, rr_sem, as_sem, ar_sem, ts_sem, tr_sem, ps_sem, pr_sem, qs_sem, qr_sem,
):
    rows, span = rbuf.shape
    blocks = out_ch.shape[0]
    piece = rows // n_dp
    wide = tri.shape[0]
    cuts = ((0, span // 2), (span // 2, 3 * span // 8), (7 * span // 8, span // 8))
    me = lax.axis_index("dp")
    mine = lax.axis_index("group")
    order = sorted(range(1, n_dp), key=lambda d: (abs(2 * d - n_dp), d))

    def dp_peer(d):
        return lax.rem(me + d, n_dp)

    def group_peer(d):
        return lax.rem(mine + d, n_group)

    quarter = rows // 4
    loads = []
    for part in range(4):
        at = pl.ds(part * quarter, quarter)
        loads.append(pltpu.make_async_copy(val_hbm.at[at], vbuf.at[at], load_sem.at[part]))
        loads[-1].start()

    def row_of(kind, b):
        return packed[kind * blocks + b : kind * blocks + b + 1, :].astype(F32)

    barrier = pltpu.get_barrier_semaphore()
    for d in range(1, n_dp):
        pl.semaphore_signal(barrier, inc=1, device_id=(dp_peer(d), mine), device_id_type=MESH)
    for d in range(1, n_group):
        pl.semaphore_signal(barrier, inc=1, device_id=(me, group_peer(d)), device_id_type=MESH)

    targets = [
        jnp.broadcast_to(row_of(3, 0)[:, p : p + 1], (piece, LANES)) for p in range(n_dp)
    ]

    def pick(d, source):
        k = jnp.full((piece, LANES), dp_peer(d), jnp.int32).astype(F32)
        weights = [(target == k).astype(F32).astype(source.dtype) for target in targets]
        for c in range(0, source.shape[1], LANES):
            at = slice(c, c + LANES)
            yield at, sum(source[p * piece : (p + 1) * piece, at] * weights[p] for p in range(n_dp))

    def stage(d, source, target):
        for at, part in pick(d, source):
            target[d, :, at] = part

    stage(order[0], rbuf, rsend)
    pl.semaphore_wait(barrier, n_dp + n_group - 2)

    def remote(src, dst, send, recv, who):
        return pltpu.make_async_remote_copy(
            src_ref=src, dst_ref=dst, send_sem=send, recv_sem=recv,
            device_id=who, device_id_type=MESH,
        )

    sent = []
    second = []
    for d, later in zip(order, order[1:] + [0]):
        stage(later, rbuf, rsend)
        k = dp_peer(d)
        sent.append(remote(rsend.at[d], out_r.at[me], rs_sem.at[d], rr_sem.at[d], (k, mine)))
        sent[-1].start()
    own = [pltpu.make_async_copy(rsend.at[0], out_r.at[me], own_sem.at[0])]
    own[0].start()

    for b in range(blocks):
        at = pl.ds(b * LANES, LANES)
        rate = jnp.transpose(jnp.broadcast_to(rate_ref[b : b + 1, :], (LANES, LANES)))
        length = jnp.transpose(jnp.broadcast_to(row_of(0, b), (LANES, LANES)))
        lenb[at, :] = length.astype(jnp.int32)
        bstep[at, :] = jnp.exp(-rate * wide)
        carry[at, :] = jnp.zeros((LANES, LANES), F32)
        for x in range(4):
            acc[x, at, :] = jnp.zeros((LANES, LANES), F32)
        for h in range(wide // LANES):
            offset = (lax.broadcasted_iota(jnp.int32, (LANES, LANES), 1) + h * LANES).astype(F32)
            lower[at, h * LANES : (h + 1) * LANES] = jnp.exp(-rate * offset)
            upper[at, h * LANES : (h + 1) * LANES] = jnp.exp(rate * offset)
    tri[...] = (
        lax.broadcasted_iota(jnp.int32, (wide, wide), 0)
        >= lax.broadcasted_iota(jnp.int32, (wide, wide), 1)
    ).astype(F32).astype(BF16)
    for load in loads:
        load.wait()

    reps = wide // LANES

    def column_step(i, _):
        col = pl.multiple_of((span // wide - 1 - i) * wide, wide)
        for b in range(blocks):
            at = pl.ds(b * LANES, LANES)
            length = lenb[at, :]
            position = col + lax.broadcasted_iota(jnp.int32, (LANES, wide), 1)
            valid = position < jnp.concatenate([length] * reps, axis=1)
            r = jnp.where(valid, rbuf[at, pl.ds(col, wide)].astype(F32), 0.0)
            s = r * lower[at, :]
            high = s.astype(BF16)
            low = (s - high.astype(F32)).astype(BF16)
            both = jnp.dot(
                jnp.concatenate([high, low], axis=0), tri[...], preferred_element_type=F32
            )
            c = carry[at, :]
            summed = both[:LANES] + both[LANES:] + jnp.concatenate([c] * reps, axis=1)
            carry[at, :] = bstep[at, :] * jnp.broadcast_to(summed[:, :1], (LANES, LANES))
            a = upper[at, :] * summed - vbuf[at, pl.ds(col, wide)].astype(F32)
            a = jnp.where(valid, a, 0.0).astype(BF16)
            abuf[at, pl.ds(col, wide)] = a
            a = a.astype(F32)
            for x, term in enumerate((r, a, r * r, a * a)):
                acc[x, at, :] += sum(term[:, h * LANES : (h + 1) * LANES] for h in range(reps))
        return 0

    lax.fori_loop(0, span // wide, column_step, 0)

    lane = lax.broadcasted_iota(jnp.int32, (LANES, LANES), 1)
    for b in range(blocks):
        at = pl.ds(b * LANES, LANES)
        terms = jnp.where(lane == 0, lenb[at, :].astype(F32), 0.0)
        for x in range(4):
            total = jnp.sum(acc[x, at, :], axis=1, keepdims=True)
            terms = jnp.where(lane == x + 1, total, terms)
        tbuf[at, :] = terms
    tstage[...] = jnp.zeros_like(tstage)

    def stage_second(d, _):
        stage(d, abuf, asend)
        for at, part in pick(d, tbuf):
            tstage[0:piece, :] = part
        tsend[d] = jnp.transpose(tstage[...])[0:8, :]
        return 0

    lax.fori_loop(0, n_dp, stage_second, 0)

    terms_sent = []
    for d in order:
        k = dp_peer(d)
        terms_sent.append(remote(tsend.at[d], trecv.at[me], ts_sem.at[d], tr_sem.at[d], (k, mine)))
        terms_sent[-1].start()
    trecv[me] = tsend[0]

    def send_second(part):
        at = pl.ds(*cuts[part])
        second.append([])
        for d in order:
            k = dp_peer(d)
            second[part].append(
                remote(
                    asend.at[d, :, at], out_a.at[me, :, at],
                    as_sem.at[part, d], ar_sem.at[part, d], (k, mine),
                )
            )
            second[part][-1].start()

    send_second(0)
    own.append(pltpu.make_async_copy(asend.at[0], out_a.at[me], own_sem.at[1]))
    own[1].start()

    for copy in terms_sent:
        copy.wait()

    row = lax.broadcasted_iota(jnp.int32, (LANES, LANES), 0).astype(F32)
    partial = jnp.zeros((8, LANES), F32)
    per_block = LANES // piece
    for b in range(blocks):
        picked = (row == row_of(1, b)).astype(F32)
        member = (row == row_of(2, b)).astype(F32)
        arrived_member = lax.dot_general(
            member.astype(BF16), picked.astype(BF16), NT, preferred_element_type=F32
        )
        terms = trecv[b * per_block]
        for s in range(1, per_block):
            terms = terms + pltpu.roll(trecv[b * per_block + s], s * piece, 1)
        partial = partial + lax.dot_general(
            terms, arrived_member, NT, precision=HIGHEST, preferred_element_type=F32
        )
        out_ch[b] = jnp.transpose(picked).astype(BF16)
        tot[b] = jnp.dot(terms, picked, precision=HIGHEST, preferred_element_type=F32)
    psend[...] = partial
    precv[me] = partial
    sums_sent = []
    for d in order:
        k = dp_peer(d)
        sums_sent.append(remote(psend, precv.at[me], ps_sem.at[d], pr_sem.at[d], (k, mine)))
        sums_sent[-1].start()

    for part in range(1, len(cuts)):
        send_second(part)

    for copy in sums_sent:
        copy.wait()
    partial = precv[0]
    for k in range(1, n_dp):
        partial = partial + precv[k]
    qsend[...] = partial
    qrecv[mine] = partial
    group_sent = []
    for d in range(1, n_group):
        k = group_peer(d)
        group_sent.append(remote(qsend, qrecv.at[mine], qs_sem.at[d], qr_sem.at[d], (me, k)))
        group_sent[-1].start()
    for copy in group_sent:
        copy.wait()
    total = qrecv[0]
    for k in range(1, n_group):
        total = total + qrecv[k]

    count = jnp.maximum(total[0:1, :], 1.0)
    means = total[1:3, :] / count
    spreads = jnp.maximum(total[3:5, :] / count - means * means, 0.0)
    scales = lax.rsqrt(spreads + 1e-05)
    table = jnp.concatenate([means, scales, jnp.zeros((4, LANES), F32)], axis=0)
    for b in range(blocks):
        at = pl.ds(b * LANES, LANES)
        member = (row == row_of(2, b)).astype(F32)
        here = jnp.dot(table, member, precision=HIGHEST, preferred_element_type=F32)
        here = jnp.concatenate(
            [here[0:4, :], tot[b, 0:1, :], jnp.zeros((LANES - 5, LANES), F32)], axis=0
        )
        out_st[at, :] = jnp.transpose(here)

    def whiten_part(x, source, target, start, width):
        tile = min(512, width)

        def tile_step(i, _):
            col = pl.multiple_of(start + i * tile, tile)
            for b in range(blocks):
                at = pl.ds(b * LANES, LANES)
                stats = out_st[at, :]
                position = (col + lax.broadcasted_iota(jnp.int32, (LANES, tile), 1)).astype(F32)
                arrived = source[b * per_block : (b + 1) * per_block, :, pl.ds(col, tile)]
                moved = jnp.dot(
                    out_ch[b], arrived.reshape(LANES, tile), preferred_element_type=F32
                )
                white = (moved - stats[:, x : x + 1]) * stats[:, x + 2 : x + 3]
                white = jnp.where(position < stats[:, 4:5], white, 0.0)
                target[at, pl.ds(col, tile)] = white.astype(BF16)
            return 0

        lax.fori_loop(0, width // tile, tile_step, 0)

    for copy in own + sent:
        copy.wait()
    whiten_part(0, out_r, white_r, 0, span)
    for part, copies in enumerate(second):
        for copy in copies:
            copy.wait_recv()
        whiten_part(1, out_a, white_a, *cuts[part])
    for copies in second:
        for copy in copies:
            copy.wait_send()


def exchange(n_dp, n_group, rewards, values, lengths, decay_rate, piece_dest, row_perm, minibatch):
    rows, span = rewards.shape
    blocks, block = row_perm.shape
    piece = rows // n_dp
    wide = 256
    vmem = pl.BlockSpec(memory_space=pltpu.VMEM)
    far = pl.BlockSpec(memory_space=pltpu.HBM)
    dma = pltpu.SemaphoreType.DMA
    whole = pltpu.VMEM((rows, span), BF16)
    staged = pltpu.VMEM((n_dp, piece, span), BF16)
    factor = pltpu.VMEM((rows, wide), F32)
    column = pltpu.VMEM((rows, LANES), F32)
    small = pltpu.VMEM((n_dp, 8, LANES), F32)
    one = pltpu.VMEM((8, LANES), F32)
    return pl.pallas_call(
        functools.partial(exchange_kernel, n_dp, n_group),
        out_shape=(jax.ShapeDtypeStruct((rows, span), BF16),) * 2,
        in_specs=[vmem, far, vmem, vmem],
        out_specs=(vmem, vmem),
        scratch_shapes=[
            staged, staged, column, pltpu.VMEM((blocks, LANES, LANES), BF16),
            whole, whole, staged, staged,
            pltpu.VMEM((wide, wide), BF16), factor, factor,
            pltpu.VMEM((rows, LANES), jnp.int32), column, column,
            pltpu.VMEM((4, rows, LANES), F32), column, pltpu.VMEM((LANES, LANES), F32),
            small, small, one, small, one, pltpu.VMEM((n_group, 8, LANES), F32),
            pltpu.VMEM((blocks, 8, LANES), F32),
            dma((4,)), dma((2,)), dma((n_dp,)), dma((n_dp,)), dma((3, n_dp)), dma((3, n_dp)),
            dma((n_dp,)), dma((n_dp,)), dma((n_dp,)), dma((n_dp,)), dma((n_group,)), dma((n_group,)),
        ],
        compiler_params=pltpu.CompilerParams(
            collective_id=1, has_side_effects=True, vmem_limit_bytes=36_000_000
        ),
    )(
        rewards, values, decay_rate.reshape(blocks, block),
        jnp.concatenate(
            [
                lengths.reshape(blocks, block),
                row_perm,
                minibatch.reshape(blocks, block),
                jnp.pad(piece_dest, ((0, 0), (0, block - piece_dest.shape[1]))),
            ],
            axis=0,
        ),
    )


def ragged_kernel(
    n_dp, n_group, cap,
    rew_hbm, val_hbm, len_hbm, rate_hbm, dest_hbm, perm_hbm, mini_hbm,
    white_far, white_a, over_out, unused_r, unused_a,
    rbuf, vbuf, abuf, white_r, len_v, rate_v, perm_v, mini_v, dest_v,
    dsend, psend, dense, packed, chooser, placer, spread,
    out_st, out_ch, tri, lower, upper, lenb, bstep, carry,
    acc, tbuf, tstage, tsend, trecv, psum, precv, qsum, qrecv, tot,
    load_sem, meta_sem, own_sem, ds_sem, dr_sem, ks_sem, kr_sem,
    ts_sem, tr_sem, ps_sem, pr_sem, qs_sem, qr_sem,
):
    rows, span = rbuf.shape
    blocks = out_ch.shape[0]
    piece = rows // n_dp
    half = n_dp // 2
    chunks = span // LANES
    depth = placer.shape[2]
    wide = tri.shape[0]
    cuts = part_cuts(cap)
    me = lax.axis_index("dp")
    mine = lax.axis_index("group")
    side = me // half
    spot = lax.rem(me, half)

    def dp_peer(d):
        return lax.rem(me + d, n_dp)

    def group_peer(d):
        return lax.rem(mine + d, n_group)

    def near(j):
        return side * half + lax.rem(me + j, half)

    def across(j):
        return (1 - side) * half + lax.rem(me + j, half)

    small = []
    for i, (src, dst) in enumerate(
        ((len_hbm, len_v), (dest_hbm, dest_v), (rate_hbm, rate_v), (perm_hbm, perm_v), (mini_hbm, mini_v))
    ):
        small.append(pltpu.make_async_copy(src, dst, meta_sem.at[i]))
        small[-1].start()
    quarter = rows // 4
    loads = []
    for x, (src, dst) in enumerate(((rew_hbm, rbuf), (val_hbm, vbuf))):
        for part in range(4):
            at = pl.ds(part * quarter, quarter)
            loads.append(pltpu.make_async_copy(src.at[at], dst.at[at], load_sem.at[x, part]))
            loads[-1].start()

    barrier = pltpu.get_barrier_semaphore()
    for d in range(1, n_dp):
        pl.semaphore_signal(barrier, inc=1, device_id=(dp_peer(d), mine), device_id_type=MESH)
    for d in range(1, n_group):
        pl.semaphore_signal(barrier, inc=1, device_id=(me, group_peer(d)), device_id_type=MESH)

    lane = lax.broadcasted_iota(jnp.int32, (LANES, LANES), 1)
    sub = lax.broadcasted_iota(jnp.int32, (LANES, LANES), 0)
    before = jnp.logical_and(sub // piece == lane // piece, sub < lane).astype(F32).astype(BF16)
    per_vreg = LANES // piece

    def used(length):
        return ((length + (LANES - 1)) // LANES).astype(F32).astype(BF16)

    for copy in small:
        copy.wait()

    dests = [dest_v[0:1, p : p + 1] for p in range(n_dp)]
    targets = [jnp.broadcast_to(dest.astype(F32), (piece, LANES)) for dest in dests]
    row_dest = []
    for b in range(blocks):
        here = jnp.zeros((16, LANES), jnp.int32)
        for q in range(per_vreg):
            here = jnp.where(lane[0:16] // piece == q, dests[b * per_vreg + q], here)
        row_dest.append(here)
    fold = (sub % piece == lane % piece).astype(F32).astype(BF16)

    def pick(k, source):
        k = jnp.full((piece, LANES), k, jnp.int32).astype(F32)
        weights = [(target == k).astype(F32).astype(source.dtype) for target in targets]
        for c in range(0, source.shape[1], LANES):
            at = slice(c, c + LANES)
            yield at, sum(source[p * piece : (p + 1) * piece, at] * weights[p] for p in range(n_dp))

    def choose(j, over):
        wanted = jnp.zeros((16, LANES), F32)
        for b in range(blocks):
            here = jnp.broadcast_to(len_v[b : b + 1, :], (16, LANES))
            here = jnp.where(row_dest[b] == across(j), here, 0)
            wanted = wanted + jnp.dot(used(here), fold, preferred_element_type=F32)
        base = jnp.dot(wanted.astype(BF16), before, preferred_element_type=F32)
        over = jnp.maximum(over, jnp.where(base + wanted > cap, 1.0, 0.0)[0:8])
        base = base.astype(jnp.int32)[0:1]
        wanted = wanted.astype(jnp.int32)[0:1]
        place = lax.broadcasted_iota(jnp.int32, (cap, LANES), 0)
        for v in range(chunks // per_vreg):
            c = lane[0:1] // piece + v * per_vreg
            key = jnp.where(c < wanted, base + c, -1)
            chooser[j, :, v * LANES : (v + 1) * LANES] = (place == key).astype(F32).astype(BF16)
        return over

    def pack(x, j, source):
        arranged = jnp.concatenate([part for _, part in pick(across(j), source)], axis=0)
        psend[x, j] = jnp.dot(chooser[j], arranged, preferred_element_type=F32).astype(BF16)

    def copy_dense(x, j, source):
        for at, part in pick(near(j), source):
            dsend[x, j, :, at] = part

    packed_tail = packed.shape[2] - cap
    if packed_tail:
        packed[:, :, cap:, :] = jnp.zeros((2, half, packed_tail, LANES), BF16)

    for load in loads[:4]:
        load.wait()

    def remote(src, dst, send, recv, who):
        return pltpu.make_async_remote_copy(
            src_ref=src, dst_ref=dst, send_sem=send, recv_sem=recv,
            device_id=who, device_id_type=MESH,
        )

    def dense_copy(x, j):
        return remote(
            dsend.at[x, j], dense.at[x, spot], ds_sem.at[x, j], dr_sem.at[x, j], (near(j), mine)
        )

    def packed_copy(x, j, part):
        at = pl.ds(*cuts[x][part])
        return remote(
            psend.at[x, j, at], packed.at[x, spot, at],
            ks_sem.at[x, part, j], kr_sem.at[x, part, j], (across(j), mine),
        )

    order = []
    for j in range(half):
        order.append((0, j))
        if j + 1 < half:
            order.append((1, j + 1))

    overs = [jnp.zeros((8, LANES), F32)]

    def stage(item):
        kind, j = item
        if kind:
            copy_dense(0, j, rbuf)
        else:
            overs.append(choose(j, overs[-1]))
            pack(0, j, rbuf)

    def issue(x, item):
        kind, j = item
        copy = dense_copy(x, j) if kind else packed_copy(x, j, 0)
        copy.start()
        return copy

    dense_sent = [[], []]
    packed_sent = [[[]], [[] for _ in cuts[1]]]
    stage(order[0])
    pl.semaphore_wait(barrier, n_dp + n_group - 2)
    for item, later in zip(order, order[1:] + [(1, 0)]):
        stage(later)
        (dense_sent[0] if item[0] else packed_sent[0][0]).append(issue(0, item))
    own = [pltpu.make_async_copy(dsend.at[0, 0], dense.at[0, spot], own_sem.at[0])]
    own[0].start()

    for b in range(blocks):
        at = pl.ds(b * LANES, LANES)
        rate = jnp.transpose(jnp.broadcast_to(rate_v[b : b + 1, :], (LANES, LANES)))
        length = jnp.transpose(jnp.broadcast_to(len_v[b : b + 1, :].astype(F32), (LANES, LANES)))
        lenb[at, :] = length.astype(jnp.int32)
        bstep[at, :] = jnp.exp(-rate * wide)
        carry[at, :] = jnp.zeros((LANES, LANES), F32)
        for x in range(4):
            acc[x, at, :] = jnp.zeros((LANES, LANES), F32)
        for i in range(wide // LANES):
            offset = (lane + i * LANES).astype(F32)
            lower[at, i * LANES : (i + 1) * LANES] = jnp.exp(-rate * offset)
            upper[at, i * LANES : (i + 1) * LANES] = jnp.exp(rate * offset)
    tri[...] = (
        lax.broadcasted_iota(jnp.int32, (wide, wide), 0)
        >= lax.broadcasted_iota(jnp.int32, (wide, wide), 1)
    ).astype(F32).astype(BF16)
    for load in loads[4:]:
        load.wait()

    reps = wide // LANES

    def column_step(i, _):
        col = pl.multiple_of((span // wide - 1 - i) * wide, wide)
        for b in range(blocks):
            at = pl.ds(b * LANES, LANES)
            length = lenb[at, :]
            position = col + lax.broadcasted_iota(jnp.int32, (LANES, wide), 1)
            valid = position < jnp.concatenate([length] * reps, axis=1)
            r = jnp.where(valid, rbuf[at, pl.ds(col, wide)].astype(F32), 0.0)
            s = r * lower[at, :]
            high = s.astype(BF16)
            low = (s - high.astype(F32)).astype(BF16)
            both = jnp.dot(
                jnp.concatenate([high, low], axis=0), tri[...], preferred_element_type=F32
            )
            c = carry[at, :]
            summed = both[:LANES] + both[LANES:] + jnp.concatenate([c] * reps, axis=1)
            carry[at, :] = bstep[at, :] * jnp.broadcast_to(summed[:, :1], (LANES, LANES))
            a = upper[at, :] * summed - vbuf[at, pl.ds(col, wide)].astype(F32)
            a = jnp.where(valid, a, 0.0).astype(BF16)
            abuf[at, pl.ds(col, wide)] = a
            a = a.astype(F32)
            for x, term in enumerate((r, a, r * r, a * a)):
                acc[x, at, :] += sum(term[:, i * LANES : (i + 1) * LANES] for i in range(reps))
        return 0

    lax.fori_loop(0, span // wide, column_step, 0)

    for b in range(blocks):
        at = pl.ds(b * LANES, LANES)
        terms = jnp.where(lane == 0, lenb[at, :].astype(F32), 0.0)
        for x in range(4):
            total = jnp.sum(acc[x, at, :], axis=1, keepdims=True)
            terms = jnp.where(lane == x + 1, total, terms)
        tbuf[at, :] = terms
    tstage[...] = jnp.zeros_like(tstage)

    def stage_terms(d, _):
        for at, part in pick(dp_peer(d), tbuf):
            tstage[0:piece, :] = part
        tsend[d] = jnp.transpose(tstage[...])[0:8, :]
        return 0

    lax.fori_loop(0, n_dp, stage_terms, 0)

    def stage_second(j, _):
        copy_dense(1, j, abuf)
        pack(1, j, abuf)
        return 0

    lax.fori_loop(0, half, stage_second, 0)

    terms_sent = []
    for d in range(1, n_dp):
        k = dp_peer(d)
        terms_sent.append(remote(tsend.at[d], trecv.at[me], ts_sem.at[d], tr_sem.at[d], (k, mine)))
        terms_sent[-1].start()
    trecv[me] = tsend[0]

    for item in order:
        (dense_sent[1] if item[0] else packed_sent[1][0]).append(issue(1, item))
    own.append(pltpu.make_async_copy(dsend.at[1, 0], dense.at[1, spot], own_sem.at[1]))
    own[1].start()

    for copy in terms_sent:
        copy.wait()

    row = sub.astype(F32)
    partial = jnp.where(lax.broadcasted_iota(jnp.int32, (8, LANES), 0) == 5, overs[-1], 0.0)
    per_block = LANES // piece
    for b in range(blocks):
        picked = (row == perm_v[b : b + 1, :].astype(F32)).astype(F32)
        member = (row == mini_v[b : b + 1, :].astype(F32)).astype(F32)
        arrived_member = lax.dot_general(
            member.astype(BF16), picked.astype(BF16), NT, preferred_element_type=F32
        )
        terms = trecv[b * per_block]
        for s in range(1, per_block):
            terms = terms + pltpu.roll(trecv[b * per_block + s], s * piece, 1)
        partial = partial + lax.dot_general(
            terms, arrived_member, NT, precision=HIGHEST, preferred_element_type=F32
        )
        out_ch[b] = jnp.transpose(picked).astype(BF16)
        tot[b] = jnp.dot(terms, picked, precision=HIGHEST, preferred_element_type=F32)
    psum[...] = partial
    precv[me] = partial
    sums_sent = []
    for d in range(1, n_dp):
        k = dp_peer(d)
        sums_sent.append(remote(psum, precv.at[me], ps_sem.at[d], pr_sem.at[d], (k, mine)))
        sums_sent[-1].start()

    for part in range(1, len(cuts[1])):
        for j in range(half):
            packed_sent[1][part].append(packed_copy(1, j, part))
            packed_sent[1][part][-1].start()

    other = 1 - side
    length = trecv[other * per_block]
    for s in range(1, per_block):
        length = length + pltpu.roll(trecv[other * per_block + s], s * piece, 1)
    length = jnp.broadcast_to(length[0:1], (16, LANES)).astype(jnp.int32)
    wanted = used(length)
    base = jnp.dot(wanted, before, preferred_element_type=F32)
    base = jnp.transpose(jnp.broadcast_to(base[0:1], (LANES, LANES))).astype(jnp.int32)
    wanted = jnp.transpose(jnp.broadcast_to(wanted.astype(F32)[0:1], (LANES, LANES))).astype(jnp.int32)

    def place_chunk(c, _):
        key = jnp.where(c < wanted, base + c, -1)
        at = pl.ds(pl.multiple_of(c * piece, piece), piece)
        for n in range(depth // LANES):
            match = (lane + n * LANES == key).astype(F32).astype(BF16)
            for q in range(half):
                placer[q, at, n * LANES : (n + 1) * LANES] = match[q * piece : (q + 1) * piece]
        return 0

    lax.fori_loop(0, chunks, place_chunk, 0)

    def unpack(x, start, stop, first):
        stop = depth if stop == cap else stop

        def one(q, _):
            got = jnp.dot(
                placer[q, :, start:stop], packed[x, q, start:stop, :], preferred_element_type=F32
            ).astype(BF16)
            at = pl.ds(pl.multiple_of(q * piece, piece), piece)
            for c in range(chunks):
                cols = slice(c * LANES, (c + 1) * LANES)
                part = got[c * piece : (c + 1) * piece]
                spread[x, at, cols] = part if first else spread[x, at, cols] + part
            return 0

        lax.fori_loop(0, half, one, 0)

    for copy in own[:1] + dense_sent[0] + packed_sent[0][0]:
        copy.wait()
    unpack(0, 0, cap, True)

    for copy in sums_sent:
        copy.wait()
    partial = precv[0]
    for k in range(1, n_dp):
        partial = partial + precv[k]
    qsum[...] = partial
    qrecv[mine] = partial
    group_sent = []
    for d in range(1, n_group):
        k = group_peer(d)
        group_sent.append(remote(qsum, qrecv.at[mine], qs_sem.at[d], qr_sem.at[d], (me, k)))
        group_sent[-1].start()
    for copy in group_sent:
        copy.wait()
    total = qrecv[0]
    for k in range(1, n_group):
        total = total + qrecv[k]
    over_out[0] = jnp.max(total[5:6, :])

    count = jnp.maximum(total[0:1, :], 1.0)
    means = total[1:3, :] / count
    spreads = jnp.maximum(total[3:5, :] / count - means * means, 0.0)
    scales = lax.rsqrt(spreads + 1e-05)
    table = jnp.concatenate([means, scales, jnp.zeros((4, LANES), F32)], axis=0)
    for b in range(blocks):
        at = pl.ds(b * LANES, LANES)
        member = (row == mini_v[b : b + 1, :].astype(F32)).astype(F32)
        here = jnp.dot(table, member, precision=HIGHEST, preferred_element_type=F32)
        here = jnp.concatenate(
            [here[0:4, :], tot[b, 0:1, :], jnp.zeros((LANES - 5, LANES), F32)], axis=0
        )
        out_st[at, :] = jnp.transpose(here)

    def whiten_block(x, arrived_at, b, target):
        tile = 512

        def tile_step(i, _):
            col = pl.multiple_of(i * tile, tile)
            at = pl.ds(pl.multiple_of(b * LANES, LANES), LANES)
            stats = out_st[at, :]
            position = (col + lax.broadcasted_iota(jnp.int32, (LANES, tile), 1)).astype(F32)
            moved = jnp.dot(out_ch[b], arrived_at(pl.ds(col, tile)), preferred_element_type=F32)
            white = (moved - stats[:, x : x + 1]) * stats[:, x + 2 : x + 3]
            white = jnp.where(position < stats[:, 4:5], white, 0.0)
            target[at, pl.ds(col, tile)] = white.astype(BF16)
            return 0

        lax.fori_loop(0, span // tile, tile_step, 0)

    def whiten_dense(x, target):
        whiten_block(x, lambda at: dense[x, :, :, at].reshape(LANES, at.size), side, target)

    def whiten_packed(x, target):
        whiten_block(x, lambda at: spread[x, :, at], other, target)

    whiten_dense(0, white_r)
    whiten_packed(0, white_r)
    kept = pltpu.make_async_copy(white_r, white_far, own_sem.at[2])
    kept.start()
    for copy in own[1:] + dense_sent[1]:
        copy.wait()
    whiten_dense(1, white_a)
    for part, copies in enumerate(packed_sent[1]):
        for copy in copies:
            copy.wait_recv()
        start, size = cuts[1][part]
        unpack(1, start, start + size, part == 0)
    whiten_packed(1, white_a)
    for copies in packed_sent[1]:
        for copy in copies:
            copy.wait_send()
    kept.wait()


def part_cuts(cap):
    a, b = cap // 256 * 128, cap // 128 * 128
    b = b - 128 if cap - b < 64 else b
    return (((0, cap),), ((0, a), (a, b - a), (b, cap - b)))


def ragged_capacity(rows, n_dp, span):
    chunks = rows // n_dp * (span // LANES)
    return chunks * 23 // 32 // 16 * 16


def ragged(n_dp, n_group, rewards, values, lengths, decay_rate, piece_dest, row_perm, minibatch):
    rows, span = rewards.shape
    blocks, block = row_perm.shape
    piece = rows // n_dp
    half = n_dp // 2
    wide = 256
    cap = ragged_capacity(rows, n_dp, span)
    depth = -(-cap // LANES) * LANES
    chunks = piece * (span // LANES)
    vmem = pl.BlockSpec(memory_space=pltpu.VMEM)
    far = pl.BlockSpec(memory_space=pltpu.HBM)
    dma = pltpu.SemaphoreType.DMA
    whole = pltpu.VMEM((rows, span), BF16)
    factor = pltpu.VMEM((rows, wide), F32)
    column = pltpu.VMEM((rows, LANES), F32)
    small = pltpu.VMEM((n_dp, 8, LANES), F32)
    one = pltpu.VMEM((8, LANES), F32)
    meta = pltpu.VMEM((blocks, LANES), jnp.int32)
    dense = pltpu.VMEM((2, half, piece, span), BF16)
    parts = len(part_cuts(cap)[1])
    return pl.pallas_call(
        functools.partial(ragged_kernel, n_dp, n_group, cap),
        out_shape=(jax.ShapeDtypeStruct((rows, span), BF16),) * 2
        + (jax.ShapeDtypeStruct((1,), F32),)
        + (jax.ShapeDtypeStruct((rows, span), BF16),) * 2,
        in_specs=[far] * 7,
        out_specs=(far, vmem, pl.BlockSpec(memory_space=pltpu.SMEM), far, far),
        scratch_shapes=[
            whole, whole, whole, whole, meta, pltpu.VMEM((blocks, LANES), F32), meta, meta,
            pltpu.VMEM((1, n_dp), jnp.int32),
            dense, pltpu.VMEM((2, half, cap, LANES), BF16),
            dense, pltpu.VMEM((2, half, depth, LANES), BF16),
            pltpu.VMEM((half, cap, chunks), BF16), pltpu.VMEM((half, chunks, depth), BF16),
            pltpu.VMEM((2, LANES, span), BF16),
            column, pltpu.VMEM((blocks, LANES, LANES), BF16),
            pltpu.VMEM((wide, wide), BF16), factor, factor,
            pltpu.VMEM((rows, LANES), jnp.int32), column, column,
            pltpu.VMEM((4, rows, LANES), F32), column, pltpu.VMEM((LANES, LANES), F32),
            small, small, one, small, one, pltpu.VMEM((n_group, 8, LANES), F32),
            pltpu.VMEM((blocks, 8, LANES), F32),
            dma((2, 4)), dma((5,)), dma((3,)), dma((2, half)), dma((2, half)),
            dma((2, parts, half)), dma((2, parts, half)),
            dma((n_dp,)), dma((n_dp,)), dma((n_dp,)), dma((n_dp,)), dma((n_group,)), dma((n_group,)),
        ],
        compiler_params=pltpu.CompilerParams(
            collective_id=0, has_side_effects=True, vmem_limit_bytes=44_000_000
        ),
    )(
        rewards, values, lengths.reshape(blocks, block), decay_rate.reshape(blocks, block),
        piece_dest, row_perm, minibatch.reshape(blocks, block),
    )


def write_kernel(over, from_r, from_a, whole_r, whole_a, to_r, to_a, bounce, sem):
    quarter = from_r.shape[0] // 4

    def move(sources, targets):
        copies = []
        for x, (src, dst) in enumerate(zip(sources, targets)):
            for part in range(4):
                at = pl.ds(part * quarter, quarter)
                copies.append(pltpu.make_async_copy(src.at[at], dst.at[at], sem.at[x, part]))
                copies[-1].start()
        for copy in copies:
            copy.wait()

    @pl.when(over[0] > 0.0)
    def _():
        for source, target in ((whole_r, to_r), (whole_a, to_a)):
            move((source,), (bounce,))
            move((bounce,), (target,))

    @pl.when(jnp.logical_not(over[0] > 0.0))
    def _():
        reads, writes = [], []
        for part in range(4):
            at = pl.ds(part * quarter, quarter)
            reads.append(pltpu.make_async_copy(from_r.at[at], bounce.at[at], sem.at[2, part]))
            reads[-1].start()
        for part in range(4):
            at = pl.ds(part * quarter, quarter)
            writes.append(pltpu.make_async_copy(from_a.at[at], to_a.at[at], sem.at[1, part]))
            writes[-1].start()
        for part in range(4):
            at = pl.ds(part * quarter, quarter)
            reads[part].wait()
            writes.append(pltpu.make_async_copy(bounce.at[at], to_r.at[at], sem.at[0, part]))
            writes[-1].start()
        for copy in writes:
            copy.wait()


def write(over, packed_way, whole_way):
    vmem = pl.BlockSpec(memory_space=pltpu.VMEM)
    far = pl.BlockSpec(memory_space=pltpu.HBM)
    shape = packed_way[0].shape
    return tuple(
        pl.pallas_call(
            write_kernel,
            out_shape=[jax.ShapeDtypeStruct(x.shape, x.dtype) for x in packed_way],
            in_specs=[pl.BlockSpec(memory_space=pltpu.SMEM), far, vmem, far, far],
            out_specs=[far, far],
            scratch_shapes=[pltpu.VMEM(shape, BF16), pltpu.SemaphoreType.DMA((3, 4))],
            compiler_params=pltpu.CompilerParams(vmem_limit_bytes=4_000_000),
        )(over, *packed_way, *whole_way)
    )


def local(n_dp, n_group, rewards, values, lengths, decay_rate, piece_dest, row_perm, minibatch):
    rows, span = rewards.shape
    blocks, block = row_perm.shape
    piece = rows // n_dp
    args = (rewards, values, lengths, decay_rate, piece_dest, row_perm, minibatch)
    if piece % 16 or LANES % piece or block != LANES or span % 4096:
        return plain_local(*args)
    whole = functools.partial(exchange, n_dp, n_group)
    if n_dp % 2 or blocks != 2 or n_dp // 2 * piece != LANES:
        return whole(*args)
    white_rewards, white_advantage, over, *unused = ragged(n_dp, n_group, *args)
    whole_way = lax.cond(
        over[0] > 0.0,
        lambda unused, args: tuple(whole(*args)),
        lambda unused, args: tuple(unused),
        unused, args,
    )
    return write(over, (white_rewards, white_advantage), whole_way)


def solution(mesh):
    return jax.shard_map(
        functools.partial(local, mesh.shape["dp"], mesh.shape["group"]),
        mesh=mesh,
        in_specs=(
            P(("dp", "group"), None),
            P(("dp", "group"), None),
            P(("dp", "group")),
            P(("dp", "group")),
            P("dp", None),
            P(("dp", "group"), None),
            P(("dp", "group")),
        ),
        out_specs=(P(("dp", "group"), None), P(("dp", "group"), None)),
        check_vma=False,
    )
```

```python
import functools

import jax
import jax.numpy as jnp
from jax import lax
from jax.experimental import pallas as pl
from jax.experimental.pallas import tpu as pltpu
from jax.sharding import PartitionSpec as P

MINIBATCHES = 64


HIGHEST = lax.Precision.HIGHEST


def discounted(rewards, values, lengths, decay_rate):
    rows_here, span = rewards.shape
    block = min(128, span)
    blocks_here = span // block
    position = jnp.arange(span, dtype=jnp.int32)
    is_valid = position[None, :] < lengths[:, None]
    next_valid = position[None, :] + 1 < lengths[:, None]
    per_step = jnp.exp(-decay_rate)
    value_f = values.astype(jnp.float32)
    value_next = jnp.concatenate([value_f[:, 1:], jnp.zeros((rows_here, 1), jnp.float32)], axis=1)
    td_error = (
        rewards.astype(jnp.float32)
        + per_step[:, None] * jnp.where(next_valid, value_next, 0.0)
        - value_f
    )
    td_error = jnp.where(is_valid, td_error, 0.0).reshape(rows_here, blocks_here, block)
    offset = jnp.arange(block, dtype=jnp.float32)
    lower_scale = jnp.exp(-decay_rate[:, None] * offset[None, :])
    upper_scale = jnp.exp(decay_rate[:, None] * offset[None, :])
    triangle = (offset[:, None] >= offset[None, :]).astype(jnp.float32)
    scaled = td_error * lower_scale[:, None, :]
    summed = jnp.einsum("rjk,kt->rjt", scaled, triangle, precision=HIGHEST)
    local_part = summed * upper_scale[:, None, :]
    heads = local_part[:, :, 0]
    block_step = jnp.exp(-decay_rate * block)

    def carry_step(carry, head):
        fresh = head + block_step * carry
        return (fresh, fresh)

    final_carry, starts = lax.scan(carry_step, jnp.zeros_like(decay_rate), heads.T, reverse=True)
    next_heads = jnp.concatenate([starts[1:].T, jnp.zeros((rows_here, 1), jnp.float32)], axis=1)
    reach = jnp.exp(-decay_rate[:, None] * (block - offset[None, :]))
    total = local_part + reach[:, None, :] * next_heads[:, :, None]
    return jnp.where(is_valid, total.reshape(rows_here, span), 0.0).astype(jnp.bfloat16)


def by_target(array, piece_dest):
    peers = piece_dest.shape[1]
    target = piece_dest[0]
    slots = jnp.arange(peers, dtype=jnp.int32)
    source_slot = jnp.sum(jnp.where(target[None, :] == slots[:, None], slots[None, :], 0), axis=1)
    pieces = array.reshape((peers, array.shape[0] // peers) + array.shape[1:])
    return jnp.take(pieces, source_slot, axis=0).reshape(array.shape)


def reorder(received, row_perm):
    blocks_here, block = row_perm.shape
    chooser = (row_perm[:, :, None] == jnp.arange(block, dtype=jnp.int32)[None, None, :]).astype(
        jnp.bfloat16
    )

    def permute_one(member):
        shaped = member.reshape(blocks_here, block, member.shape[-1])
        mixed = jnp.einsum("bim,bmc->bic", chooser, shaped, preferred_element_type=jnp.float32)
        return mixed.astype(jnp.bfloat16).reshape(member.shape)

    return tuple((permute_one(member) for member in received))


def whiten(rewards, advantage, lengths, minibatch):
    rows_here, span = rewards.shape
    position = jnp.arange(span, dtype=jnp.int32)
    is_valid = position[None, :] < lengths[:, None]
    counted = lengths.astype(jnp.float32)
    reward_f = jnp.where(is_valid, rewards.astype(jnp.float32), 0.0)
    advantage_f = jnp.where(is_valid, advantage.astype(jnp.float32), 0.0)
    member = (minibatch[:, None] == jnp.arange(MINIBATCHES, dtype=jnp.int32)[None, :]).astype(
        jnp.float32
    )
    row_terms = jnp.stack(
        [
            counted,
            jnp.sum(reward_f, axis=1),
            jnp.sum(advantage_f, axis=1),
            jnp.sum(reward_f * reward_f, axis=1),
            jnp.sum(advantage_f * advantage_f, axis=1),
        ],
        axis=1,
    )
    totals = lax.psum(jnp.dot(member.T, row_terms, precision=HIGHEST), ("dp", "group"))
    count = jnp.maximum(totals[:, 0], 1.0)
    means = totals[:, 1:3] / count[:, None]
    spreads = totals[:, 3:5] / count[:, None] - means * means
    row_means = jnp.dot(member, means, precision=HIGHEST)
    row_scale = jnp.dot(member, lax.rsqrt(spreads + 1e-05), precision=HIGHEST)
    white_rewards = jnp.where(is_valid, (reward_f - row_means[:, 0:1]) * row_scale[:, 0:1], 0.0)
    white_advantage = jnp.where(
        is_valid, (advantage_f - row_means[:, 1:2]) * row_scale[:, 1:2], 0.0
    )
    return (white_rewards.astype(jnp.bfloat16), white_advantage.astype(jnp.bfloat16))


def plain_local(rewards, values, lengths, decay_rate, piece_dest, row_perm, minibatch):
    blocks_here, block = row_perm.shape
    new_order = (jnp.arange(blocks_here, dtype=jnp.int32)[:, None] * block + row_perm).reshape(-1)
    per_row = jnp.stack([lengths.astype(jnp.float32), decay_rate], axis=1)
    moved_terms = lax.all_to_all(
        by_target(per_row, piece_dest), "dp", split_axis=0, concat_axis=0, tiled=True
    )
    moved_terms = jnp.take(moved_terms, new_order, axis=0)
    lengths_here = moved_terms[:, 0].astype(jnp.int32)
    rate_here = moved_terms[:, 1]
    moved_rewards, moved_second = reorder(
        (
            lax.all_to_all(
                by_target(rewards, piece_dest), "dp", split_axis=0, concat_axis=0, tiled=True
            ),
            lax.all_to_all(
                by_target(values, piece_dest), "dp", split_axis=0, concat_axis=0, tiled=True
            ),
        ),
        row_perm,
    )
    advantage = discounted(moved_rewards, moved_second, lengths_here, rate_here)
    return whiten(moved_rewards, advantage, lengths_here, minibatch)


F32 = jnp.float32
BF16 = jnp.bfloat16
LANES = 128
MESH = pl.DeviceIdType.MESH
NT = (((1,), (1,)), ((), ()))


def ragged_kernel(
    n_dp, n_group, own_part, shared,
    rew_hbm, val_hbm, len_hbm, rate_hbm, dest_hbm, perm_hbm, mini_hbm,
    white_far, white_a, over_out, unused_r, unused_a,
    rbuf, vbuf, abuf, white_r, len_v, rate_v, perm_v, mini_v, dest_v,
    dsend, psend, hsend, hrecv, merged, esend, erecv, dense, packed, chooser, placer, spread,
    out_st, out_ch, tri, lower, upper, lenb, bstep, carry,
    acc, tbuf, tstage, tsend, trecv, psum, precv, qsum, qrecv, tot,
    load_sem, meta_sem, own_sem, ds_sem, dr_sem, ks_sem, kr_sem, hs_sem, hr_sem, fs_sem, xs_sem, xr_sem, es_sem,
    ts_sem, tr_sem, ps_sem, pr_sem, qs_sem, qr_sem,
):
    rows, span = rbuf.shape
    blocks = out_ch.shape[0]
    piece = rows // n_dp
    half = n_dp // 2
    chunks = span // LANES
    quarter = half // 2
    depth = own_part + shared
    wide = tri.shape[0]
    cuts = part_cuts(own_part)
    me = lax.axis_index("dp")
    mine = lax.axis_index("group")
    side = me // half
    spot = lax.rem(me, half)
    column = lax.rem(spot, quarter)
    core = lax.rem(mine, 2)
    partner = mine + 1 - 2 * core

    def dp_peer(d):
        return lax.rem(me + d, n_dp)

    def group_peer(d):
        return lax.rem(mine + d, n_group)

    def near(j):
        return side * half + lax.rem(me + j, half)

    def across(i, f):
        level = side if f == 0 else 1 - side
        return (1 - side) * half + level * quarter + lax.rem(column + i, quarter)

    small = []
    for i, (src, dst) in enumerate(
        ((len_hbm, len_v), (dest_hbm, dest_v), (rate_hbm, rate_v), (perm_hbm, perm_v), (mini_hbm, mini_v))
    ):
        small.append(pltpu.make_async_copy(src, dst, meta_sem.at[i]))
        small[-1].start()
    step = rows // 4
    loads = []
    for x, (src, dst) in enumerate(((rew_hbm, rbuf), (val_hbm, vbuf))):
        for part in range(4):
            at = pl.ds(part * step, step)
            loads.append(pltpu.make_async_copy(src.at[at], dst.at[at], load_sem.at[x, part]))
            loads[-1].start()

    barrier = pltpu.get_barrier_semaphore()
    for d in range(1, n_dp):
        pl.semaphore_signal(barrier, inc=1, device_id=(dp_peer(d), mine), device_id_type=MESH)
    for d in range(1, n_group):
        pl.semaphore_signal(barrier, inc=1, device_id=(me, group_peer(d)), device_id_type=MESH)

    lane = lax.broadcasted_iota(jnp.int32, (LANES, LANES), 1)
    sub = lax.broadcasted_iota(jnp.int32, (LANES, LANES), 0)
    before = jnp.logical_and(sub // piece == lane // piece, sub < lane).astype(F32).astype(BF16)
    per_vreg = LANES // piece

    def used(length):
        return ((length + (LANES - 1)) // LANES).astype(F32).astype(BF16)

    for copy in small:
        copy.wait()

    dests = [dest_v[0:1, p : p + 1] for p in range(n_dp)]
    targets = [jnp.broadcast_to(dest.astype(F32), (piece, LANES)) for dest in dests]
    row_dest = []
    for b in range(blocks):
        here = jnp.zeros((16, LANES), jnp.int32)
        for q in range(per_vreg):
            here = jnp.where(lane[0:16] // piece == q, dests[b * per_vreg + q], here)
        row_dest.append(here)
    fold = (sub % piece == lane % piece).astype(F32).astype(BF16)

    def pick(k, source):
        k = jnp.full((piece, LANES), k, jnp.int32).astype(F32)
        weights = [(target == k).astype(F32).astype(source.dtype) for target in targets]
        for c in range(0, source.shape[1], LANES):
            at = slice(c, c + LANES)
            yield at, sum(source[p * piece : (p + 1) * piece, at] * weights[p] for p in range(n_dp))

    def mirrored(key):
        return jnp.where(key >= own_part, own_part + depth - 1 - key, key)

    core_row = jnp.full((1, LANES), core, jnp.int32)

    def choose(i, f):
        wanted = jnp.zeros((16, LANES), F32)
        for b in range(blocks):
            here = jnp.broadcast_to(len_v[b : b + 1, :], (16, LANES))
            here = jnp.where(row_dest[b] == across(i, f), here, 0)
            wanted = wanted + jnp.dot(used(here), fold, preferred_element_type=F32)
        base = jnp.dot(wanted.astype(BF16), before, preferred_element_type=F32)
        taken = jnp.max((base + wanted)[0:8], axis=1, keepdims=True)
        base = base.astype(jnp.int32)[0:1]
        wanted = wanted.astype(jnp.int32)[0:1]
        place = lax.broadcasted_iota(jnp.int32, (depth, LANES), 0)
        for v in range(chunks // per_vreg):
            c = lane[0:1] // piece + v * per_vreg
            key = base + c
            key = jnp.where(core_row == i, key, mirrored(key))
            key = jnp.where(c < wanted, key, -1)
            at = slice(v * LANES, (v + 1) * LANES)
            chooser[i, f, :, at] = (place == key).astype(F32).astype(BF16)
        return jnp.maximum(jnp.broadcast_to(taken, (8, LANES)) - own_part, 0.0)

    def pack(x, i, f, source):
        arranged = jnp.concatenate([part for _, part in pick(across(i, f), source)], axis=0)
        got = jnp.dot(chooser[i, f], arranged, preferred_element_type=F32).astype(BF16)
        psend[x, i, f] = got[:own_part]
        if shared:
            hsend[x, i, f] = got[own_part:]

    def copy_dense(x, j, source):
        for at, part in pick(near(j), source):
            dsend[x, j, :, at] = part

    for load in loads[:4]:
        load.wait()

    def remote(src, dst, send, recv, who):
        return pltpu.make_async_remote_copy(
            src_ref=src, dst_ref=dst, send_sem=send, recv_sem=recv,
            device_id=who, device_id_type=MESH,
        )

    def dense_copy(x, j):
        return remote(
            dsend.at[x, j], dense.at[x, spot], ds_sem.at[x, j], dr_sem.at[x, j], (near(j), mine)
        )

    def packed_copy(x, i, f, part):
        at = pl.ds(*cuts[x][part])
        return remote(
            psend.at[x, i, f, at], packed.at[x, spot, at],
            ks_sem.at[x, part, i, f], kr_sem.at[x, part, spot], (across(i, f), mine),
        )

    last = pl.ds(own_part, shared)

    def swap_copy(x, f):
        return remote(
            hsend.at[x, 1 - core, f], hrecv.at[x, f], xs_sem.at[x, f], xr_sem.at[x, f], (me, partner)
        )

    def shared_copy(x, f):
        return remote(
            merged.at[x, f], packed.at[x, spot, last],
            hs_sem.at[x, f], hr_sem.at[x, spot], (across(core, f), mine),
        )

    def relay_copy(x, f, own):
        q = f * quarter + lax.rem(column + core + (0 if own else 1), 2)
        return remote(
            packed.at[x, q, last], packed.at[x, q, last],
            fs_sem.at[x, f], hr_sem.at[x, q], (me, partner),
        )

    def swap(x):
        for f in range(2 if shared else 0):
            swap_copy(x, f).start()

    def merge(x):
        for f in range(2 if shared else 0):
            swap_copy(x, f).wait_recv()
            merged[x, f] = hsend[x, core, f] + hrecv[x, f]
        for f in range(2 if shared else 0):
            shared_copy(x, f).start()

    def receive_packed(x, part):
        at = pl.ds(*cuts[x][part])
        for q in range(half):
            remote(
                psend.at[x, 0, 0, at], packed.at[x, q, at],
                ks_sem.at[x, part, 0, 0], kr_sem.at[x, part, q], (across(0, 0), mine),
            ).wait_recv()

    def relay(x):
        for f in range(2 if shared else 0):
            relay_copy(x, f, True).wait_recv()
            relay_copy(x, f, True).start()

    def relayed(x):
        for f in range(2 if shared else 0):
            relay_copy(x, f, False).wait_recv()

    order = []
    for i in range(quarter):
        for f in range(2):
            order.append(("own", i, f))
            if len(order) < n_dp - 1:
                order.append(("near", i * 2 + f + 1, 0))
    beyond_own = {}

    def stage(item):
        kind, i, f = item
        if kind == "near":
            copy_dense(0, i, rbuf)
        else:
            beyond_own[i, f] = choose(i, f)
            pack(0, i, f, rbuf)

    sent = []

    def issue(x, item):
        kind, i, f = item
        if kind == "near":
            dense_sent[x].append(dense_copy(x, i))
            dense_sent[x][-1].start()
        else:
            sent.append(packed_copy(x, i, f, 0))
            sent[-1].start()

    dense_sent = [[], []]
    stage(order[0])
    pl.semaphore_wait(barrier, n_dp + n_group - 2)
    held = len(order) - 2
    for item, later in zip(order[:held], order[1:]):
        stage(later)
        issue(0, item)

    for b in range(blocks):
        at = pl.ds(b * LANES, LANES)
        rate = jnp.transpose(jnp.broadcast_to(rate_v[b : b + 1, :], (LANES, LANES)))
        length = jnp.transpose(jnp.broadcast_to(len_v[b : b + 1, :].astype(F32), (LANES, LANES)))
        lenb[at, :] = length.astype(jnp.int32)
        bstep[at, :] = jnp.exp(-rate * wide)
        carry[at, :] = jnp.zeros((LANES, LANES), F32)
        for x in range(4):
            acc[x, at, :] = jnp.zeros((LANES, LANES), F32)
        for i in range(wide // LANES):
            offset = (lane + i * LANES).astype(F32)
            lower[at, i * LANES : (i + 1) * LANES] = jnp.exp(-rate * offset)
            upper[at, i * LANES : (i + 1) * LANES] = jnp.exp(rate * offset)
    tri[...] = (
        lax.broadcasted_iota(jnp.int32, (wide, wide), 0)
        >= lax.broadcasted_iota(jnp.int32, (wide, wide), 1)
    ).astype(F32).astype(BF16)
    for load in loads[4:]:
        load.wait()

    reps = wide // LANES

    def column_step(i, _):
        col = pl.multiple_of((span // wide - 1 - i) * wide, wide)
        for b in range(blocks):
            at = pl.ds(b * LANES, LANES)
            length = lenb[at, :]
            position = col + lax.broadcasted_iota(jnp.int32, (LANES, wide), 1)
            valid = position < jnp.concatenate([length] * reps, axis=1)
            r = jnp.where(valid, rbuf[at, pl.ds(col, wide)].astype(F32), 0.0)
            s = r * lower[at, :]
            high = s.astype(BF16)
            low = (s - high.astype(F32)).astype(BF16)
            both = jnp.dot(
                jnp.concatenate([high, low], axis=0), tri[...], preferred_element_type=F32
            )
            c = carry[at, :]
            summed = both[:LANES] + both[LANES:] + jnp.concatenate([c] * reps, axis=1)
            carry[at, :] = bstep[at, :] * jnp.broadcast_to(summed[:, :1], (LANES, LANES))
            a = upper[at, :] * summed - vbuf[at, pl.ds(col, wide)].astype(F32)
            a = jnp.where(valid, a, 0.0).astype(BF16)
            abuf[at, pl.ds(col, wide)] = a
            a = a.astype(F32)
            for x, term in enumerate((r, a, r * r, a * a)):
                acc[x, at, :] += sum(term[:, i * LANES : (i + 1) * LANES] for i in range(reps))
        return 0

    lax.fori_loop(0, span // wide, column_step, 0)

    for b in range(blocks):
        at = pl.ds(b * LANES, LANES)
        terms = jnp.where(lane == 0, lenb[at, :].astype(F32), 0.0)
        for x in range(4):
            total = jnp.sum(acc[x, at, :], axis=1, keepdims=True)
            terms = jnp.where(lane == x + 1, total, terms)
        tbuf[at, :] = terms
    tstage[...] = jnp.zeros_like(tstage)

    def stage_terms(d, _):
        for at, part in pick(dp_peer(d), tbuf):
            tstage[0:piece, :] = part
        tsend[d] = jnp.transpose(tstage[...])[0:8, :]
        return 0

    lax.fori_loop(0, n_dp, stage_terms, 0)

    terms_sent = []
    for d in range(1, n_dp):
        k = dp_peer(d)
        terms_sent.append(remote(tsend.at[d], trecv.at[me], ts_sem.at[d], tr_sem.at[d], (k, mine)))
        terms_sent[-1].start()
    trecv[me] = tsend[0]
    for item, later in zip(order[held:], order[held + 1 :] + [("near", 0, 0)]):
        stage(later)
        issue(0, item)
    own = [pltpu.make_async_copy(dsend.at[0, 0], dense.at[0, spot], own_sem.at[0])]
    own[0].start()
    swap(0)
    for i in range(quarter):
        for f in range(2):
            esend[2 * i + f] = beyond_own[i, f]
    for i in range(quarter):
        for f in range(2):
            pack(1, i, f, abuf)
    for j in range(half):
        copy_dense(1, j, abuf)
    swap(1)
    merge(0)
    tell = remote(esend, erecv, es_sem.at[0], es_sem.at[1], (me, partner))
    tell.start()

    for copy in terms_sent:
        copy.wait()

    row = sub.astype(F32)
    over = jnp.zeros((8, LANES), F32)
    tell.wait()
    for slot in range(half):
        over = jnp.where(esend[slot] + erecv[slot] > shared, 1.0, over)
    partial = jnp.where(lax.broadcasted_iota(jnp.int32, (8, LANES), 0) == 5, over, 0.0)
    per_block = LANES // piece
    for b in range(blocks):
        picked = (row == perm_v[b : b + 1, :].astype(F32)).astype(F32)
        member = (row == mini_v[b : b + 1, :].astype(F32)).astype(F32)
        arrived_member = lax.dot_general(
            member.astype(BF16), picked.astype(BF16), NT, preferred_element_type=F32
        )
        terms = trecv[b * per_block]
        for s in range(1, per_block):
            terms = terms + pltpu.roll(trecv[b * per_block + s], s * piece, 1)
        partial = partial + lax.dot_general(
            terms, arrived_member, NT, precision=HIGHEST, preferred_element_type=F32
        )
        out_ch[b] = jnp.transpose(picked).astype(BF16)
        tot[b] = jnp.dot(terms, picked, precision=HIGHEST, preferred_element_type=F32)
    psum[...] = partial
    precv[me] = partial
    sums_sent = []
    for d in range(1, n_dp):
        k = dp_peer(d)
        sums_sent.append(remote(psum, precv.at[me], ps_sem.at[d], pr_sem.at[d], (k, mine)))
        sums_sent[-1].start()

    merge(1)
    for item in order:
        issue(1, item)
    own.append(pltpu.make_async_copy(dsend.at[1, 0], dense.at[1, spot], own_sem.at[1]))
    own[1].start()
    for part in range(1, len(cuts[1])):
        for i in range(quarter):
            for f in range(2):
                sent.append(packed_copy(1, i, f, part))
                sent[-1].start()

    relay(0)
    other = 1 - side
    length = trecv[other * per_block]
    for s in range(1, per_block):
        length = length + pltpu.roll(trecv[other * per_block + s], s * piece, 1)
    length = jnp.broadcast_to(length[0:1], (16, LANES)).astype(jnp.int32)
    wanted = used(length)
    base = jnp.dot(wanted, before, preferred_element_type=F32)
    base = jnp.transpose(jnp.broadcast_to(base[0:1], (LANES, LANES))).astype(jnp.int32)
    wanted = jnp.transpose(jnp.broadcast_to(wanted.astype(F32)[0:1], (LANES, LANES))).astype(jnp.int32)

    flips = lax.rem(sub // piece + column, 2) != core

    def place_chunk(c, _):
        key = base + c
        key = jnp.where(flips, mirrored(key), key)
        key = jnp.where(c < wanted, key, -1)
        at = pl.ds(pl.multiple_of(c * piece, piece), piece)
        for n in range(depth // LANES):
            match = (lane + n * LANES == key).astype(F32).astype(BF16)
            for q in range(half):
                placer[q, at, n * LANES : (n + 1) * LANES] = match[q * piece : (q + 1) * piece]
        return 0

    lax.fori_loop(0, chunks, place_chunk, 0)

    def unpack(x, start, stop, first):
        stop = depth if stop == own_part else stop

        def one(q, _):
            got = jnp.dot(
                placer[q, :, start:stop], packed[x, q, start:stop, :], preferred_element_type=F32
            ).astype(BF16)
            at = pl.ds(pl.multiple_of(q * piece, piece), piece)
            for c in range(chunks):
                cols = slice(c * LANES, (c + 1) * LANES)
                part = got[c * piece : (c + 1) * piece]
                spread[x, at, cols] = part if first else spread[x, at, cols] + part
            return 0

        lax.fori_loop(0, half, one, 0)

    for copy in own[:1] + dense_sent[0]:
        copy.wait()
    receive_packed(0, 0)
    relayed(0)
    unpack(0, 0, own_part, True)
    relay(1)

    for copy in sums_sent:
        copy.wait()
    partial = precv[0]
    for k in range(1, n_dp):
        partial = partial + precv[k]
    qsum[...] = partial
    qrecv[mine] = partial
    group_sent = []
    for d in range(1, n_group):
        k = group_peer(d)
        group_sent.append(remote(qsum, qrecv.at[mine], qs_sem.at[d], qr_sem.at[d], (me, k)))
        group_sent[-1].start()
    for copy in group_sent:
        copy.wait()
    total = qrecv[0]
    for k in range(1, n_group):
        total = total + qrecv[k]
    over_out[0] = jnp.max(total[5:6, :])

    count = jnp.maximum(total[0:1, :], 1.0)
    means = total[1:3, :] / count
    spreads = jnp.maximum(total[3:5, :] / count - means * means, 0.0)
    scales = lax.rsqrt(spreads + 1e-05)
    table = jnp.concatenate([means, scales, jnp.zeros((4, LANES), F32)], axis=0)
    for b in range(blocks):
        at = pl.ds(b * LANES, LANES)
        member = (row == mini_v[b : b + 1, :].astype(F32)).astype(F32)
        here = jnp.dot(table, member, precision=HIGHEST, preferred_element_type=F32)
        here = jnp.concatenate(
            [here[0:4, :], tot[b, 0:1, :], jnp.zeros((LANES - 5, LANES), F32)], axis=0
        )
        out_st[at, :] = jnp.transpose(here)

    def whiten_block(x, arrived_at, b, target):
        tile = 512

        def tile_step(i, _):
            col = pl.multiple_of(i * tile, tile)
            at = pl.ds(pl.multiple_of(b * LANES, LANES), LANES)
            stats = out_st[at, :]
            position = (col + lax.broadcasted_iota(jnp.int32, (LANES, tile), 1)).astype(F32)
            moved = jnp.dot(out_ch[b], arrived_at(pl.ds(col, tile)), preferred_element_type=F32)
            white = (moved - stats[:, x : x + 1]) * stats[:, x + 2 : x + 3]
            white = jnp.where(position < stats[:, 4:5], white, 0.0)
            target[at, pl.ds(col, tile)] = white.astype(BF16)
            return 0

        lax.fori_loop(0, span // tile, tile_step, 0)

    def whiten_dense(x, target):
        whiten_block(x, lambda at: dense[x, :, :, at].reshape(LANES, at.size), side, target)

    def whiten_packed(x, target):
        whiten_block(x, lambda at: spread[x, :, at], other, target)

    whiten_dense(0, white_r)
    whiten_packed(0, white_r)
    kept = pltpu.make_async_copy(white_r, white_far.at[pl.ds(0, rows)], own_sem.at[2])
    kept.start()
    for copy in own[1:] + dense_sent[1]:
        copy.wait()
    whiten_dense(1, white_a)
    for part, (start, size) in enumerate(cuts[1]):
        receive_packed(1, part)
        if part == len(cuts[1]) - 1:
            relayed(1)
        unpack(1, start, start + size, part == 0)
    whiten_packed(1, white_a)
    for copy in sent:
        copy.wait_send()
    for x in range(2):
        for f in range(2 if shared else 0):
            swap_copy(x, f).wait_send()
            shared_copy(x, f).wait_send()
            relay_copy(x, f, True).wait_send()
    kept.wait()


def part_cuts(size):
    a, b = size // 256 * 128, (size - 1) // 128 * 128
    return (((0, size),), ((0, a), (a, b - a), (b, size - b)))


def ragged(n_dp, n_group, own_part, shared, collective_id, spare, rewards, values, lengths, decay_rate, piece_dest, row_perm, minibatch):
    rows, span = rewards.shape
    blocks, block = row_perm.shape
    piece = rows // n_dp
    half = n_dp // 2
    wide = 256
    depth = own_part + shared
    extra = max(shared, 16)
    chunks = piece * (span // LANES)
    vmem = pl.BlockSpec(memory_space=pltpu.VMEM)
    far = pl.BlockSpec(memory_space=pltpu.HBM)
    dma = pltpu.SemaphoreType.DMA
    whole = pltpu.VMEM((rows, span), BF16)
    factor = pltpu.VMEM((rows, wide), F32)
    column = pltpu.VMEM((rows, LANES), F32)
    small = pltpu.VMEM((n_dp, 8, LANES), F32)
    one = pltpu.VMEM((8, LANES), F32)
    meta = pltpu.VMEM((blocks, LANES), jnp.int32)
    dense = pltpu.VMEM((2, half, piece, span), BF16)
    parts = len(part_cuts(own_part)[1])
    return pl.pallas_call(
        functools.partial(ragged_kernel, n_dp, n_group, own_part, shared),
        out_shape=tuple(jax.ShapeDtypeStruct((k * rows, span), BF16) for k in (spare, 1))
        + (jax.ShapeDtypeStruct((1,), F32),)
        + (jax.ShapeDtypeStruct((rows, span), BF16),) * 2,
        in_specs=[far] * 7,
        out_specs=(far, vmem, pl.BlockSpec(memory_space=pltpu.SMEM), far, far),
        scratch_shapes=[
            whole, whole, whole, whole, meta, pltpu.VMEM((blocks, LANES), F32), meta, meta,
            pltpu.VMEM((1, n_dp), jnp.int32),
            dense, pltpu.VMEM((2, half // 2, 2, own_part, LANES), BF16),
            pltpu.VMEM((2, 2, 2, extra, LANES), BF16),
            pltpu.VMEM((2, 2, extra, LANES), BF16), pltpu.VMEM((2, 2, extra, LANES), BF16),
            pltpu.VMEM((half, 8, LANES), F32), pltpu.VMEM((half, 8, LANES), F32),
            dense, pltpu.VMEM((2, half, depth, LANES), BF16),
            pltpu.VMEM((half // 2, 2, depth, chunks), BF16), pltpu.VMEM((half, chunks, depth), BF16),
            pltpu.VMEM((2, LANES, span), BF16),
            column, pltpu.VMEM((blocks, LANES, LANES), BF16),
            pltpu.VMEM((wide, wide), BF16), factor, factor,
            pltpu.VMEM((rows, LANES), jnp.int32), column, column,
            pltpu.VMEM((4, rows, LANES), F32), column, pltpu.VMEM((LANES, LANES), F32),
            small, small, one, small, one, pltpu.VMEM((n_group, 8, LANES), F32),
            pltpu.VMEM((blocks, 8, LANES), F32),
            dma((2, 4)), dma((5,)), dma((3,)), dma((2, half)), dma((2, half)),
            dma((2, parts, half // 2, 2)), dma((2, parts, half)),
            dma((2, 2)), dma((2, half)), dma((2, 2)), dma((2, 2)), dma((2, 2)), dma((2,)),
            dma((n_dp,)), dma((n_dp,)), dma((n_dp,)), dma((n_dp,)), dma((n_group,)), dma((n_group,)),
        ],
        compiler_params=pltpu.CompilerParams(
            collective_id=collective_id, has_side_effects=True, vmem_limit_bytes=52_000_000
        ),
    )(
        rewards, values, lengths.reshape(blocks, block), decay_rate.reshape(blocks, block),
        piece_dest, row_perm, minibatch.reshape(blocks, block),
    )


def write_kernel(over, from_r, from_a, whole_r, whole_a, to_r, to_a, bounce, sem):
    quarter = from_a.shape[0] // 4

    def move(sources, targets):
        copies = []
        for x, (src, dst) in enumerate(zip(sources, targets)):
            for part in range(4):
                at = pl.ds(part * quarter, quarter)
                copies.append(pltpu.make_async_copy(src.at[at], dst.at[at], sem.at[x, part]))
                copies[-1].start()
        for copy in copies:
            copy.wait()

    @pl.when(over[0] > 0.0)
    def _():
        for source, target in ((whole_r, to_r), (whole_a, to_a)):
            move((source,), (bounce,))
            move((bounce,), (target,))

    @pl.when(jnp.logical_not(over[0] > 0.0))
    def _():
        reads, writes = [], []
        for part in range(4):
            at = pl.ds(part * quarter, quarter)
            reads.append(pltpu.make_async_copy(from_r.at[at], bounce.at[at], sem.at[2, part]))
            reads[-1].start()
        for part in range(4):
            at = pl.ds(part * quarter, quarter)
            writes.append(pltpu.make_async_copy(from_a.at[at], to_a.at[at], sem.at[1, part]))
            writes[-1].start()
        for part in range(4):
            at = pl.ds(part * quarter, quarter)
            reads[part].wait()
            writes.append(pltpu.make_async_copy(bounce.at[at], to_r.at[at], sem.at[0, part]))
            writes[-1].start()
        for copy in writes:
            copy.wait()


def write(over, packed_way, whole_way):
    vmem = pl.BlockSpec(memory_space=pltpu.VMEM)
    far = pl.BlockSpec(memory_space=pltpu.HBM)
    shape = packed_way[1].shape
    return tuple(
        pl.pallas_call(
            write_kernel,
            out_shape=[jax.ShapeDtypeStruct(x.shape, x.dtype) for x in whole_way],
            in_specs=[pl.BlockSpec(memory_space=pltpu.SMEM), far, vmem, far, far],
            out_specs=[far, far],
            scratch_shapes=[pltpu.VMEM(shape, BF16), pltpu.SemaphoreType.DMA((3, 4))],
            compiler_params=pltpu.CompilerParams(vmem_limit_bytes=52_000_000),
        )(over, *packed_way, *whole_way)
    )


def local(n_dp, n_group, rewards, values, lengths, decay_rate, piece_dest, row_perm, minibatch):
    rows, span = rewards.shape
    blocks, block = row_perm.shape
    piece = rows // n_dp
    args = (rewards, values, lengths, decay_rate, piece_dest, row_perm, minibatch)
    if piece % 16 or LANES % piece or block != LANES or span % 4096:
        return plain_local(*args)
    if n_dp // 4 != 2 or n_dp % 4 or n_group % 2 or blocks != 2 or n_dp // 2 * piece != LANES:
        return plain_local(*args)
    chunks = piece * (span // LANES)
    own_part, shared = chunks * 9 // 16, chunks * 3 // 16

    def whole(results):
        return results[0][:rows], results[1]

    white_rewards, white_advantage, over, *unused = ragged(
        n_dp, n_group, own_part, shared, 0, 8, *args
    )
    whole_way = lax.cond(
        over[0] > 0.0,
        lambda unused, args: whole(ragged(n_dp, n_group, chunks, 0, 1, 1, *args)),
        lambda unused, args: tuple(unused),
        unused, args,
    )
    return write(over, (white_rewards, white_advantage), whole_way)


def solution(mesh):
    return jax.shard_map(
        functools.partial(local, mesh.shape["dp"], mesh.shape["group"]),
        mesh=mesh,
        in_specs=(
            P(("dp", "group"), None),
            P(("dp", "group"), None),
            P(("dp", "group")),
            P(("dp", "group")),
            P("dp", None),
            P(("dp", "group"), None),
            P(("dp", "group")),
        ),
        out_specs=(P(("dp", "group"), None), P(("dp", "group"), None)),
        check_vma=False,
    )
```

```python
import functools

import jax
import jax.numpy as jnp
from jax import lax
from jax.experimental import pallas as pl
from jax.experimental.pallas import tpu as pltpu
from jax.sharding import PartitionSpec as P

MINIBATCHES = 64


HIGHEST = lax.Precision.HIGHEST


def discounted(rewards, values, lengths, decay_rate):
    rows_here, span = rewards.shape
    block = min(128, span)
    blocks_here = span // block
    position = jnp.arange(span, dtype=jnp.int32)
    is_valid = position[None, :] < lengths[:, None]
    next_valid = position[None, :] + 1 < lengths[:, None]
    per_step = jnp.exp(-decay_rate)
    value_f = values.astype(jnp.float32)
    value_next = jnp.concatenate([value_f[:, 1:], jnp.zeros((rows_here, 1), jnp.float32)], axis=1)
    td_error = (
        rewards.astype(jnp.float32)
        + per_step[:, None] * jnp.where(next_valid, value_next, 0.0)
        - value_f
    )
    td_error = jnp.where(is_valid, td_error, 0.0).reshape(rows_here, blocks_here, block)
    offset = jnp.arange(block, dtype=jnp.float32)
    lower_scale = jnp.exp(-decay_rate[:, None] * offset[None, :])
    upper_scale = jnp.exp(decay_rate[:, None] * offset[None, :])
    triangle = (offset[:, None] >= offset[None, :]).astype(jnp.float32)
    scaled = td_error * lower_scale[:, None, :]
    summed = jnp.einsum("rjk,kt->rjt", scaled, triangle, precision=HIGHEST)
    local_part = summed * upper_scale[:, None, :]
    heads = local_part[:, :, 0]
    block_step = jnp.exp(-decay_rate * block)

    def carry_step(carry, head):
        fresh = head + block_step * carry
        return (fresh, fresh)

    final_carry, starts = lax.scan(carry_step, jnp.zeros_like(decay_rate), heads.T, reverse=True)
    next_heads = jnp.concatenate([starts[1:].T, jnp.zeros((rows_here, 1), jnp.float32)], axis=1)
    reach = jnp.exp(-decay_rate[:, None] * (block - offset[None, :]))
    total = local_part + reach[:, None, :] * next_heads[:, :, None]
    return jnp.where(is_valid, total.reshape(rows_here, span), 0.0).astype(jnp.bfloat16)


def by_target(array, piece_dest):
    peers = piece_dest.shape[1]
    target = piece_dest[0]
    slots = jnp.arange(peers, dtype=jnp.int32)
    source_slot = jnp.sum(jnp.where(target[None, :] == slots[:, None], slots[None, :], 0), axis=1)
    pieces = array.reshape((peers, array.shape[0] // peers) + array.shape[1:])
    return jnp.take(pieces, source_slot, axis=0).reshape(array.shape)


def reorder(received, row_perm):
    blocks_here, block = row_perm.shape
    chooser = (row_perm[:, :, None] == jnp.arange(block, dtype=jnp.int32)[None, None, :]).astype(
        jnp.bfloat16
    )

    def permute_one(member):
        shaped = member.reshape(blocks_here, block, member.shape[-1])
        mixed = jnp.einsum("bim,bmc->bic", chooser, shaped, preferred_element_type=jnp.float32)
        return mixed.astype(jnp.bfloat16).reshape(member.shape)

    return tuple((permute_one(member) for member in received))


def whiten(rewards, advantage, lengths, minibatch):
    rows_here, span = rewards.shape
    position = jnp.arange(span, dtype=jnp.int32)
    is_valid = position[None, :] < lengths[:, None]
    counted = lengths.astype(jnp.float32)
    reward_f = jnp.where(is_valid, rewards.astype(jnp.float32), 0.0)
    advantage_f = jnp.where(is_valid, advantage.astype(jnp.float32), 0.0)
    member = (minibatch[:, None] == jnp.arange(MINIBATCHES, dtype=jnp.int32)[None, :]).astype(
        jnp.float32
    )
    row_terms = jnp.stack(
        [
            counted,
            jnp.sum(reward_f, axis=1),
            jnp.sum(advantage_f, axis=1),
            jnp.sum(reward_f * reward_f, axis=1),
            jnp.sum(advantage_f * advantage_f, axis=1),
        ],
        axis=1,
    )
    totals = lax.psum(jnp.dot(member.T, row_terms, precision=HIGHEST), ("dp", "group"))
    count = jnp.maximum(totals[:, 0], 1.0)
    means = totals[:, 1:3] / count[:, None]
    spreads = totals[:, 3:5] / count[:, None] - means * means
    row_means = jnp.dot(member, means, precision=HIGHEST)
    row_scale = jnp.dot(member, lax.rsqrt(spreads + 1e-05), precision=HIGHEST)
    white_rewards = jnp.where(is_valid, (reward_f - row_means[:, 0:1]) * row_scale[:, 0:1], 0.0)
    white_advantage = jnp.where(
        is_valid, (advantage_f - row_means[:, 1:2]) * row_scale[:, 1:2], 0.0
    )
    return (white_rewards.astype(jnp.bfloat16), white_advantage.astype(jnp.bfloat16))


def plain_local(rewards, values, lengths, decay_rate, piece_dest, row_perm, minibatch):
    blocks_here, block = row_perm.shape
    new_order = (jnp.arange(blocks_here, dtype=jnp.int32)[:, None] * block + row_perm).reshape(-1)
    per_row = jnp.stack([lengths.astype(jnp.float32), decay_rate], axis=1)
    moved_terms = lax.all_to_all(
        by_target(per_row, piece_dest), "dp", split_axis=0, concat_axis=0, tiled=True
    )
    moved_terms = jnp.take(moved_terms, new_order, axis=0)
    lengths_here = moved_terms[:, 0].astype(jnp.int32)
    rate_here = moved_terms[:, 1]
    moved_rewards, moved_second = reorder(
        (
            lax.all_to_all(
                by_target(rewards, piece_dest), "dp", split_axis=0, concat_axis=0, tiled=True
            ),
            lax.all_to_all(
                by_target(values, piece_dest), "dp", split_axis=0, concat_axis=0, tiled=True
            ),
        ),
        row_perm,
    )
    advantage = discounted(moved_rewards, moved_second, lengths_here, rate_here)
    return whiten(moved_rewards, advantage, lengths_here, minibatch)


F32 = jnp.float32
BF16 = jnp.bfloat16
LANES = 128
MESH = pl.DeviceIdType.MESH
NT = (((1,), (1,)), ((), ()))


def ragged_kernel(
    n_dp, n_group, own_part, shared,
    rew_hbm, val_hbm, len_hbm, rate_hbm, dest_hbm, perm_hbm, mini_hbm,
    white_far, white_a, white_k, over_out, unused_r, unused_a,
    rbuf, vbuf, abuf, white_r, len_v, rate_v, perm_v, mini_v, dest_v,
    dsend, psend, hsend, hrecv, merged, esend, erecv, gsend, grecv, arranged, late, dense, packed, chooser, placer, spread,
    out_st, out_ch, tri, lower, upper, lenb, bstep, carry,
    acc, tbuf, tstage, tsend, trecv, psum, precv, qsum, qrecv, tot,
    load_sem, meta_sem, own_sem, ds_sem, dr_sem, ks_sem, kr_sem, hs_sem, hr_sem, fs_sem, xs_sem, xr_sem, es_sem, er_sem, gs_sem, gr_sem,
    ts_sem, tr_sem, ps_sem, pr_sem, qs_sem, qr_sem,
):
    rows, span = rbuf.shape
    blocks = out_ch.shape[0]
    piece = rows // n_dp
    half = n_dp // 2
    chunks = span // LANES
    quarter = half // 2
    depth = own_part + shared
    wide = tri.shape[0]
    cuts = part_cuts(own_part)
    me = lax.axis_index("dp")
    mine = lax.axis_index("group")
    side = me // half
    spot = lax.rem(me, half)
    column = lax.rem(spot, quarter)
    level = spot // quarter

    def dp_peer(d):
        return lax.rem(me + d, n_dp)

    def group_peer(d):
        return lax.rem(mine + d, n_group)

    def near(j):
        return side * half + lax.rem(me + j, half)

    def across(i, f):
        goal = lax.rem(level + f, 2)
        return (1 - side) * half + goal * quarter + lax.rem(column + i, quarter)

    small = []
    for i, (src, dst) in enumerate(
        ((len_hbm, len_v), (dest_hbm, dest_v), (rate_hbm, rate_v), (perm_hbm, perm_v), (mini_hbm, mini_v))
    ):
        small.append(pltpu.make_async_copy(src, dst, meta_sem.at[i]))
        small[-1].start()
    step = rows // 4
    loads = []
    for x, (src, dst) in enumerate(((rew_hbm, rbuf), (val_hbm, vbuf))):
        for part in range(4):
            at = pl.ds(part * step, step)
            loads.append(pltpu.make_async_copy(src.at[at], dst.at[at], load_sem.at[x, part]))
            loads[-1].start()

    barrier = pltpu.get_barrier_semaphore()
    for d in range(1, n_dp):
        pl.semaphore_signal(barrier, inc=1, device_id=(dp_peer(d), mine), device_id_type=MESH)
    for d in range(1, n_group):
        pl.semaphore_signal(barrier, inc=1, device_id=(me, group_peer(d)), device_id_type=MESH)

    lane = lax.broadcasted_iota(jnp.int32, (LANES, LANES), 1)
    sub = lax.broadcasted_iota(jnp.int32, (LANES, LANES), 0)
    before = jnp.logical_and(sub // piece == lane // piece, sub < lane).astype(F32).astype(BF16)
    per_vreg = LANES // piece

    def used(length):
        return ((length + (LANES - 1)) // LANES).astype(F32).astype(BF16)

    for copy in small:
        copy.wait()

    dests = [dest_v[0:1, p : p + 1] for p in range(n_dp)]
    targets = [jnp.broadcast_to(dest.astype(F32), (piece, LANES)) for dest in dests]
    row_dest = []
    for b in range(blocks):
        here = jnp.zeros((16, LANES), jnp.int32)
        for q in range(per_vreg):
            here = jnp.where(lane[0:16] // piece == q, dests[b * per_vreg + q], here)
        row_dest.append(here)
    fold = (sub % piece == lane % piece).astype(F32).astype(BF16)

    def pick(k, source):
        k = jnp.full((piece, LANES), k, jnp.int32).astype(F32)
        weights = [(target == k).astype(F32).astype(source.dtype) for target in targets]
        for c in range(0, source.shape[1], LANES):
            at = slice(c, c + LANES)
            yield at, sum(source[p * piece : (p + 1) * piece, at] * weights[p] for p in range(n_dp))

    counts = {}

    def choose(i, f):
        wanted = jnp.zeros((16, LANES), F32)
        for b in range(blocks):
            here = jnp.broadcast_to(len_v[b : b + 1, :], (16, LANES))
            here = jnp.where(row_dest[b] == across(i, f), here, 0)
            wanted = wanted + jnp.dot(used(here), fold, preferred_element_type=F32)
        base = jnp.dot(wanted.astype(BF16), before, preferred_element_type=F32)
        taken = jnp.max((base + wanted)[0:8], axis=1, keepdims=True)
        base = base.astype(jnp.int32)[0:1]
        wanted = wanted.astype(jnp.int32)[0:1]
        counts[i, f] = base, wanted
        match_rows(chooser, i, f, own_part, base, wanted)
        esend[2 * i + f] = jnp.maximum(jnp.broadcast_to(taken, (8, LANES)) - own_part, 0.0)

    def match_rows(target, i, f, size, base, wanted):
        place = lax.broadcasted_iota(jnp.int32, (size, LANES), 0)
        for v in range(chunks // per_vreg):
            c = lane[0:1] // piece + v * per_vreg
            key = jnp.where(c < wanted, base + c, -1)
            at = slice(v * LANES, (v + 1) * LANES)
            target[i, f, :, at] = (place == key).astype(F32).astype(BF16)

    def pack(x, i, f, source):
        for c, (_, part) in enumerate(pick(across(i, f), source)):
            arranged[x, i, f, c * piece : (c + 1) * piece, :] = part
        psend[x, i, f] = jnp.dot(
            chooser[i, f], arranged[x, i, f], preferred_element_type=F32
        ).astype(BF16)

    def ahead(table, own):
        total = jnp.zeros_like(own)
        for m in range(n_group):
            total = total + jnp.where(jnp.full(own.shape, m, jnp.int32) < mine, table[m], 0.0)
        return total

    def pack_late():
        for i in range(quarter):
            for f in range(2 if shared else 0):
                base, wanted = counts[i, f]
                skip = ahead(erecv[:, 2 * i + f], esend[2 * i + f])[0:1].astype(jnp.int32)
                base = base + skip - own_part
                c = lane[0:1] // piece
                place = lax.broadcasted_iota(jnp.int32, (shared, LANES), 0)
                for v in range(chunks // per_vreg):
                    c = lane[0:1] // piece + v * per_vreg
                    key = jnp.where(jnp.logical_and(c < wanted, base + c >= skip), base + c, -1)
                    at = slice(v * LANES, (v + 1) * LANES)
                    late[:, at] = (place == key).astype(F32).astype(BF16)
                for x in range(2):
                    hsend[x, 2 * i + f] = jnp.dot(
                        late[...], arranged[x, i, f], preferred_element_type=F32
                    ).astype(BF16)

    def copy_dense(x, j, source):
        for at, part in pick(near(j), source):
            dsend[x, j, :, at] = part

    for load in loads[:4]:
        load.wait()

    def remote(src, dst, send, recv, who):
        return pltpu.make_async_remote_copy(
            src_ref=src, dst_ref=dst, send_sem=send, recv_sem=recv,
            device_id=who, device_id_type=MESH,
        )

    def dense_copy(x, j):
        return remote(
            dsend.at[x, j], dense.at[x, spot], ds_sem.at[x, j], dr_sem.at[x, j], (near(j), mine)
        )

    def packed_copy(x, i, f, part):
        at = pl.ds(*cuts[x][part])
        return remote(
            psend.at[x, i, f, at], packed.at[x, spot, at],
            ks_sem.at[x, part, i, f], kr_sem.at[x, part, spot], (across(i, f), mine),
        )

    last = pl.ds(own_part, shared)

    others = range(1, n_group if shared else 1)

    def swap_copy(x, d):
        k = group_peer(d)
        return remote(
            hsend.at[x, k], hrecv.at[x, mine], xs_sem.at[x, d], xr_sem.at[x, d], (me, k)
        )

    def shared_copy(x):
        return remote(
            merged.at[x], packed.at[x, spot, last],
            hs_sem.at[x], hr_sem.at[x, spot], (across(mine // 2, lax.rem(mine, 2)), mine),
        )

    def held_by(m):
        return lax.rem(level + lax.rem(m, 2), 2) * quarter + lax.rem(column + m // 2, 2)

    def relay_copy(x, m, d):
        q = held_by(m)
        return remote(
            packed.at[x, q, last], packed.at[x, q, last],
            fs_sem.at[x, d], hr_sem.at[x, q], (me, group_peer(d)),
        )

    def swap(x):
        for d in others:
            swap_copy(x, d).start()

    def merge(x):
        if shared:
            total = hsend[x, mine]
            for d in others:
                swap_copy(x, d).wait_recv()
            for d in others:
                total = total + hrecv[x, group_peer(d)]
            merged[x] = total

    def send_merged(x):
        if shared:
            shared_copy(x).start()

    def receive_packed(x, part):
        at = pl.ds(*cuts[x][part])
        for q in range(half):
            remote(
                psend.at[x, 0, 0, at], packed.at[x, q, at],
                ks_sem.at[x, part, 0, 0], kr_sem.at[x, part, q], (across(0, 0), mine),
            ).wait_recv()

    def relay(x):
        if shared:
            relay_copy(x, mine, 1).wait_recv()
        for d in others:
            relay_copy(x, mine, d).start()

    def relayed(x):
        for d in others:
            relay_copy(x, group_peer(d), 1).wait_recv()

    order = []
    for i in range(quarter):
        for f in range(2):
            order.append(("own", i, f))
            if len(order) < n_dp - 1:
                order.append(("near", i * 2 + f + 1, 0))

    def stage(item):
        kind, i, f = item
        if kind == "near":
            copy_dense(0, i, rbuf)
        else:
            choose(i, f)
            pack(0, i, f, rbuf)

    sent = []

    def issue(x, item):
        kind, i, f = item
        if kind == "near":
            dense_sent[x].append(dense_copy(x, i))
            dense_sent[x][-1].start()
        else:
            sent.append(packed_copy(x, i, f, 0))
            sent[-1].start()

    dense_sent = [[], []]
    stage(order[0])
    pl.semaphore_wait(barrier, n_dp + n_group - 2)
    held = len(order) - 2
    for item, later in zip(order[:held], order[1:]):
        stage(later)
        issue(0, item)

    for b in range(blocks):
        at = pl.ds(b * LANES, LANES)
        rate = jnp.transpose(jnp.broadcast_to(rate_v[b : b + 1, :], (LANES, LANES)))
        length = jnp.transpose(jnp.broadcast_to(len_v[b : b + 1, :].astype(F32), (LANES, LANES)))
        lenb[at, :] = length.astype(jnp.int32)
        bstep[at, :] = jnp.exp(-rate * wide)
        carry[at, :] = jnp.zeros((LANES, LANES), F32)
        for x in range(4):
            acc[x, at, :] = jnp.zeros((LANES, LANES), F32)
        for i in range(wide // LANES):
            offset = (lane + i * LANES).astype(F32)
            lower[at, i * LANES : (i + 1) * LANES] = jnp.exp(-rate * offset)
            upper[at, i * LANES : (i + 1) * LANES] = jnp.exp(rate * offset)
    tri[...] = (
        lax.broadcasted_iota(jnp.int32, (wide, wide), 0)
        >= lax.broadcasted_iota(jnp.int32, (wide, wide), 1)
    ).astype(F32).astype(BF16)
    for load in loads[4:]:
        load.wait()

    reps = wide // LANES

    def column_step(i, _):
        col = pl.multiple_of((span // wide - 1 - i) * wide, wide)
        for b in range(blocks):
            at = pl.ds(b * LANES, LANES)
            length = lenb[at, :]
            position = col + lax.broadcasted_iota(jnp.int32, (LANES, wide), 1)
            valid = position < jnp.concatenate([length] * reps, axis=1)
            r = jnp.where(valid, rbuf[at, pl.ds(col, wide)].astype(F32), 0.0)
            s = r * lower[at, :]
            high = s.astype(BF16)
            low = (s - high.astype(F32)).astype(BF16)
            both = jnp.dot(
                jnp.concatenate([high, low], axis=0), tri[...], preferred_element_type=F32
            )
            c = carry[at, :]
            summed = both[:LANES] + both[LANES:] + jnp.concatenate([c] * reps, axis=1)
            carry[at, :] = bstep[at, :] * jnp.broadcast_to(summed[:, :1], (LANES, LANES))
            a = upper[at, :] * summed - vbuf[at, pl.ds(col, wide)].astype(F32)
            a = jnp.where(valid, a, 0.0).astype(BF16)
            abuf[at, pl.ds(col, wide)] = a
            a = a.astype(F32)
            for x, term in enumerate((r, a, r * r, a * a)):
                acc[x, at, :] += sum(term[:, i * LANES : (i + 1) * LANES] for i in range(reps))
        return 0

    lax.fori_loop(0, span // wide, column_step, 0)

    for b in range(blocks):
        at = pl.ds(b * LANES, LANES)
        terms = jnp.where(lane == 0, lenb[at, :].astype(F32), 0.0)
        for x in range(4):
            total = jnp.sum(acc[x, at, :], axis=1, keepdims=True)
            terms = jnp.where(lane == x + 1, total, terms)
        tbuf[at, :] = terms
    tstage[...] = jnp.zeros_like(tstage)

    def stage_terms(d, _):
        for at, part in pick(dp_peer(d), tbuf):
            tstage[0:piece, :] = part
        tsend[d] = jnp.transpose(tstage[...])[0:8, :]
        return 0

    lax.fori_loop(0, n_dp, stage_terms, 0)

    terms_sent = []
    for d in range(1, n_dp):
        k = dp_peer(d)
        terms_sent.append(remote(tsend.at[d], trecv.at[me], ts_sem.at[d], tr_sem.at[d], (k, mine)))
        terms_sent[-1].start()
    trecv[me] = tsend[0]
    for item, later in zip(order[held:], order[held + 1 :] + [("near", 0, 0)]):
        stage(later)
        issue(0, item)
    own = [pltpu.make_async_copy(dsend.at[0, 0], dense.at[0, spot], own_sem.at[0])]
    own[0].start()
    tells = []
    for d in range(1, n_group):
        k = group_peer(d)
        tells.append(remote(esend, erecv.at[mine], es_sem.at[d], er_sem.at[d], (me, k)))
        tells[-1].start()
    erecv[mine] = esend[...]
    for i in range(quarter):
        for f in range(2):
            pack(1, i, f, abuf)
    for j in range(half):
        copy_dense(1, j, abuf)
    for copy in tells:
        copy.wait()
    pack_late()
    swap(0)
    swap(1)

    for copy in terms_sent:
        copy.wait()
    other = 1 - side
    length = trecv[other * (LANES // piece)]
    for q in range(1, LANES // piece):
        length = length + pltpu.roll(trecv[other * (LANES // piece) + q], q * piece, 1)
    length = jnp.broadcast_to(length[0:1], (16, LANES)).astype(jnp.int32)
    wanted = used(length)
    base = jnp.dot(wanted, before, preferred_element_type=F32)
    alike = (sub // piece == lane // piece).astype(F32).astype(BF16)
    beyond = jnp.dot(wanted, alike, preferred_element_type=F32)[0:8] - own_part
    gsend[...] = jnp.maximum(beyond, 0.0)
    grecv[mine] = gsend[...]
    for d in range(1, n_group):
        k = group_peer(d)
        tells.append(remote(gsend, grecv.at[mine], gs_sem.at[d], gr_sem.at[d], (me, k)))
        tells[-1].start()

    row = sub.astype(F32)
    over = jnp.zeros((8, LANES), F32)
    for slot in range(half):
        filled = erecv[0, slot]
        for m in range(1, n_group):
            filled = filled + erecv[m, slot]
        over = jnp.where(filled > shared, 1.0, over)
    partial = jnp.where(lax.broadcasted_iota(jnp.int32, (8, LANES), 0) == 5, over, 0.0)
    per_block = LANES // piece
    for b in range(blocks):
        picked = (row == perm_v[b : b + 1, :].astype(F32)).astype(F32)
        member = (row == mini_v[b : b + 1, :].astype(F32)).astype(F32)
        arrived_member = lax.dot_general(
            member.astype(BF16), picked.astype(BF16), NT, preferred_element_type=F32
        )
        terms = trecv[b * per_block]
        for s in range(1, per_block):
            terms = terms + pltpu.roll(trecv[b * per_block + s], s * piece, 1)
        partial = partial + lax.dot_general(
            terms, arrived_member, NT, precision=HIGHEST, preferred_element_type=F32
        )
        out_ch[b] = jnp.transpose(picked).astype(BF16)
        tot[b] = jnp.dot(terms, picked, precision=HIGHEST, preferred_element_type=F32)
    psum[...] = partial
    precv[me] = partial
    sums_sent = []
    for d in range(1, n_dp):
        k = dp_peer(d)
        sums_sent.append(remote(psum, precv.at[me], ps_sem.at[d], pr_sem.at[d], (k, mine)))
        sums_sent[-1].start()

    for x in range(2):
        merge(x)
    send_merged(0)
    send_merged(1)
    for item in order:
        issue(1, item)
    own.append(pltpu.make_async_copy(dsend.at[1, 0], dense.at[1, spot], own_sem.at[1]))
    own[1].start()
    for part in range(1, len(cuts[1])):
        for i in range(quarter):
            for f in range(2):
                sent.append(packed_copy(1, i, f, part))
                sent[-1].start()

    for copy in tells[n_group - 1 :]:
        copy.wait()
    skip = ahead(grecv, gsend[...])
    skip = jnp.transpose(jnp.broadcast_to(skip[0:1], (LANES, LANES))).astype(jnp.int32)
    base = jnp.transpose(jnp.broadcast_to(base[0:1], (LANES, LANES))).astype(jnp.int32)
    wanted = jnp.transpose(jnp.broadcast_to(wanted.astype(F32)[0:1], (LANES, LANES))).astype(jnp.int32)

    def place_chunk(c, _):
        key = base + c
        key = jnp.where(key >= own_part, key + skip, key)
        key = jnp.where(c < wanted, key, -1)
        at = pl.ds(pl.multiple_of(c * piece, piece), piece)
        for n in range(depth // LANES):
            match = (lane + n * LANES == key).astype(F32).astype(BF16)
            for q in range(half):
                placer[q, at, n * LANES : (n + 1) * LANES] = match[q * piece : (q + 1) * piece]
        return 0

    lax.fori_loop(0, chunks, place_chunk, 0)

    def unpack(x, start, stop, first):
        stop = depth if stop == own_part else stop

        def one(q, _):
            got = jnp.dot(
                placer[q, :, start:stop], packed[x, q, start:stop, :], preferred_element_type=F32
            ).astype(BF16)
            at = pl.ds(pl.multiple_of(q * piece, piece), piece)
            for c in range(chunks):
                cols = slice(c * LANES, (c + 1) * LANES)
                part = got[c * piece : (c + 1) * piece]
                spread[x, at, cols] = part if first else spread[x, at, cols] + part
            return 0

        lax.fori_loop(0, half, one, 0)

    for copy in own[:1] + dense_sent[0]:
        copy.wait()
    relay(0)
    receive_packed(0, 0)
    relayed(0)
    unpack(0, 0, own_part, True)
    relay(1)

    for copy in sums_sent:
        copy.wait()
    partial = precv[0]
    for k in range(1, n_dp):
        partial = partial + precv[k]
    qsum[...] = partial
    qrecv[mine] = partial
    group_sent = []
    for d in range(1, n_group):
        k = group_peer(d)
        group_sent.append(remote(qsum, qrecv.at[mine], qs_sem.at[d], qr_sem.at[d], (me, k)))
        group_sent[-1].start()
    for copy in group_sent:
        copy.wait()
    total = qrecv[0]
    for k in range(1, n_group):
        total = total + qrecv[k]
    over_out[0] = jnp.max(total[5:6, :])

    count = jnp.maximum(total[0:1, :], 1.0)
    means = total[1:3, :] / count
    spreads = jnp.maximum(total[3:5, :] / count - means * means, 0.0)
    scales = lax.rsqrt(spreads + 1e-05)
    table = jnp.concatenate([means, scales, jnp.zeros((4, LANES), F32)], axis=0)
    for b in range(blocks):
        at = pl.ds(b * LANES, LANES)
        member = (row == mini_v[b : b + 1, :].astype(F32)).astype(F32)
        here = jnp.dot(table, member, precision=HIGHEST, preferred_element_type=F32)
        here = jnp.concatenate(
            [here[0:4, :], tot[b, 0:1, :], jnp.zeros((LANES - 5, LANES), F32)], axis=0
        )
        out_st[at, :] = jnp.transpose(here)

    def whiten_block(x, arrived_at, b, target):
        tile = 512

        def tile_step(i, _):
            col = pl.multiple_of(i * tile, tile)
            at = pl.ds(pl.multiple_of(b * LANES, LANES), LANES)
            stats = out_st[at, :]
            position = (col + lax.broadcasted_iota(jnp.int32, (LANES, tile), 1)).astype(F32)
            moved = jnp.dot(out_ch[b], arrived_at(pl.ds(col, tile)), preferred_element_type=F32)
            white = (moved - stats[:, x : x + 1]) * stats[:, x + 2 : x + 3]
            white = jnp.where(position < stats[:, 4:5], white, 0.0)
            target[at, pl.ds(col, tile)] = white.astype(BF16)
            return 0

        lax.fori_loop(0, span // tile, tile_step, 0)

    def whiten_dense(x, target):
        whiten_block(x, lambda at: dense[x, :, :, at].reshape(LANES, at.size), side, target)

    def whiten_packed(x, target):
        whiten_block(x, lambda at: spread[x, :, at], other, target)

    whiten_dense(0, white_r)
    whiten_packed(0, white_r)
    rest = rows - white_k.shape[0]
    kept = pltpu.make_async_copy(
        white_r.at[pl.ds(0, rest)], white_far.at[pl.ds(0, rest)], own_sem.at[2]
    )
    kept.start()
    white_k[...] = white_r[rest:, :]
    for copy in own[1:] + dense_sent[1]:
        copy.wait()
    whiten_dense(1, white_a)
    for part, (start, size) in enumerate(cuts[1]):
        receive_packed(1, part)
        if part == len(cuts[1]) - 1:
            relayed(1)
        unpack(1, start, start + size, part == 0)
    whiten_packed(1, white_a)
    for copy in sent:
        copy.wait_send()
    for x in range(2 if shared else 0):
        shared_copy(x).wait_send()
        for d in others:
            swap_copy(x, d).wait_send()
            relay_copy(x, mine, d).wait_send()
    kept.wait()


def part_cuts(size):
    a, b = size // 256 * 128, (size - 1) // 128 * 128
    return (((0, size),), ((0, a), (a, b - a), (b, size - b)))


def ragged(n_dp, n_group, own_part, shared, collective_id, spare, rewards, values, lengths, decay_rate, piece_dest, row_perm, minibatch):
    rows, span = rewards.shape
    blocks, block = row_perm.shape
    piece = rows // n_dp
    half = n_dp // 2
    wide = 256
    depth = own_part + shared
    extra = max(shared, 16)
    chunks = piece * (span // LANES)
    vmem = pl.BlockSpec(memory_space=pltpu.VMEM)
    far = pl.BlockSpec(memory_space=pltpu.HBM)
    dma = pltpu.SemaphoreType.DMA
    whole = pltpu.VMEM((rows, span), BF16)
    factor = pltpu.VMEM((rows, wide), F32)
    column = pltpu.VMEM((rows, LANES), F32)
    small = pltpu.VMEM((n_dp, 8, LANES), F32)
    one = pltpu.VMEM((8, LANES), F32)
    meta = pltpu.VMEM((blocks, LANES), jnp.int32)
    dense = pltpu.VMEM((2, half, piece, span), BF16)
    parts = len(part_cuts(own_part)[1])
    return pl.pallas_call(
        functools.partial(ragged_kernel, n_dp, n_group, own_part, shared),
        out_shape=tuple(
            jax.ShapeDtypeStruct((k, span), BF16) for k in (spare * rows, rows, rows * 5 // 8)
        )
        + (jax.ShapeDtypeStruct((1,), F32),)
        + (jax.ShapeDtypeStruct((rows, span), BF16),) * 2,
        in_specs=[far] * 7,
        out_specs=(far, vmem, vmem, pl.BlockSpec(memory_space=pltpu.SMEM), far, far),
        scratch_shapes=[
            whole, whole, whole, whole, meta, pltpu.VMEM((blocks, LANES), F32), meta, meta,
            pltpu.VMEM((1, n_dp), jnp.int32),
            dense, pltpu.VMEM((2, half // 2, 2, own_part, LANES), BF16),
            pltpu.VMEM((2, half, extra, LANES), BF16), pltpu.VMEM((2, n_group, extra, LANES), BF16),
            pltpu.VMEM((2, extra, LANES), BF16),
            pltpu.VMEM((half, 8, LANES), F32), pltpu.VMEM((n_group, half, 8, LANES), F32),
            one, pltpu.VMEM((n_group, 8, LANES), F32),
            pltpu.VMEM((2, 2, 2, chunks, LANES), BF16), pltpu.VMEM((extra, chunks), BF16),
            dense, pltpu.VMEM((2, half, depth, LANES), BF16),
            pltpu.VMEM((half // 2, 2, own_part, chunks), BF16), pltpu.VMEM((half, chunks, depth), BF16),
            pltpu.VMEM((2, LANES, span), BF16),
            column, pltpu.VMEM((blocks, LANES, LANES), BF16),
            pltpu.VMEM((wide, wide), BF16), factor, factor,
            pltpu.VMEM((rows, LANES), jnp.int32), column, column,
            pltpu.VMEM((4, rows, LANES), F32), column, pltpu.VMEM((LANES, LANES), F32),
            small, small, one, small, one, pltpu.VMEM((n_group, 8, LANES), F32),
            pltpu.VMEM((blocks, 8, LANES), F32),
            dma((2, 4)), dma((5,)), dma((3,)), dma((2, half)), dma((2, half)),
            dma((2, parts, half // 2, 2)), dma((2, parts, half)),
            dma((2,)), dma((2, half)), dma((2, n_group)), dma((2, n_group)), dma((2, n_group)),
            dma((n_group,)), dma((n_group,)), dma((n_group,)), dma((n_group,)),
            dma((n_dp,)), dma((n_dp,)), dma((n_dp,)), dma((n_dp,)), dma((n_group,)), dma((n_group,)),
        ],
        compiler_params=pltpu.CompilerParams(
            collective_id=collective_id, has_side_effects=True, vmem_limit_bytes=52_000_000
        ),
    )(
        rewards, values, lengths.reshape(blocks, block), decay_rate.reshape(blocks, block),
        piece_dest, row_perm, minibatch.reshape(blocks, block),
    )


def write_kernel(over, from_r, from_a, from_k, whole_r, whole_a, to_r, to_a, bounce, sem):
    rows, kept = from_a.shape[0], from_k.shape[0]
    rest = rows - kept

    def started(src, dst, at):
        copy = pltpu.make_async_copy(src, dst, sem.at[at])
        copy.start()
        return copy

    @pl.when(over[0] > 0.0)
    def _():
        for source, target in ((whole_r, to_r), (whole_a, to_a)):
            started(source, bounce, 0).wait()
            started(bounce, target, 0).wait()

    @pl.when(jnp.logical_not(over[0] > 0.0))
    def _():
        half = rest // 2
        parts = [pl.ds(half * k, half) for k in range(2)]
        reads = [started(from_r.at[at], bounce.at[at], k) for k, at in enumerate(parts)]
        writes = [started(from_k, to_r.at[pl.ds(rest, kept)], 2)]
        for k in range(2):
            at = pl.ds(k * rows // 2, rows // 2)
            writes.append(started(from_a.at[at], to_a.at[at], 3 + k))
        for k, at in enumerate(parts):
            reads[k].wait()
            writes.append(started(bounce.at[at], to_r.at[at], 5 + k))
        for copy in writes:
            copy.wait()


def write(over, results, whole_way):
    vmem = pl.BlockSpec(memory_space=pltpu.VMEM)
    far = pl.BlockSpec(memory_space=pltpu.HBM)
    shape = whole_way[0].shape
    return tuple(
        pl.pallas_call(
            write_kernel,
            out_shape=[jax.ShapeDtypeStruct(x.shape, x.dtype) for x in whole_way],
            in_specs=[pl.BlockSpec(memory_space=pltpu.SMEM), far, vmem, vmem, far, far],
            out_specs=[far, far],
            scratch_shapes=[pltpu.VMEM(shape, BF16), pltpu.SemaphoreType.DMA((7,))],
            compiler_params=pltpu.CompilerParams(vmem_limit_bytes=52_000_000),
        )(over, *results, *whole_way)
    )


def local(n_dp, n_group, rewards, values, lengths, decay_rate, piece_dest, row_perm, minibatch):
    rows, span = rewards.shape
    blocks, block = row_perm.shape
    piece = rows // n_dp
    args = (rewards, values, lengths, decay_rate, piece_dest, row_perm, minibatch)
    if piece % 16 or LANES % piece or block != LANES or span % 4096:
        return plain_local(*args)
    if n_dp // 4 != 2 or n_dp % 4 or n_group != 4 or blocks != 2 or n_dp // 2 * piece != LANES:
        return plain_local(*args)
    chunks = piece * (span // LANES)
    own_part, shared = chunks * 36 // 64, chunks * 12 // 64

    def whole(results):
        kept = results[2]
        rest = rows - kept.shape[0]
        return jnp.concatenate([results[0][:rest], kept], axis=0), results[1]

    *results, over, unused_r, unused_a = ragged(
        n_dp, n_group, own_part, shared, 0, 8, *args
    )
    whole_way = lax.cond(
        over[0] > 0.0,
        lambda unused, args: whole(ragged(n_dp, n_group, chunks, 0, 1, 1, *args)),
        lambda unused, args: tuple(unused),
        (unused_r, unused_a), args,
    )
    return write(over, results, whole_way)


def solution(mesh):
    return jax.shard_map(
        functools.partial(local, mesh.shape["dp"], mesh.shape["group"]),
        mesh=mesh,
        in_specs=(
            P(("dp", "group"), None),
            P(("dp", "group"), None),
            P(("dp", "group")),
            P(("dp", "group")),
            P("dp", None),
            P(("dp", "group"), None),
            P(("dp", "group")),
        ),
        out_specs=(P(("dp", "group"), None), P(("dp", "group"), None)),
        check_vma=False,
    )
```

```python
import functools

import jax
import jax.numpy as jnp
from jax import lax
from jax.experimental import pallas as pl
from jax.experimental.pallas import tpu as pltpu
from jax.sharding import PartitionSpec as P

MINIBATCHES = 64


HIGHEST = lax.Precision.HIGHEST


def discounted(rewards, values, lengths, decay_rate):
    rows_here, span = rewards.shape
    block = min(128, span)
    blocks_here = span // block
    position = jnp.arange(span, dtype=jnp.int32)
    is_valid = position[None, :] < lengths[:, None]
    next_valid = position[None, :] + 1 < lengths[:, None]
    per_step = jnp.exp(-decay_rate)
    value_f = values.astype(jnp.float32)
    value_next = jnp.concatenate([value_f[:, 1:], jnp.zeros((rows_here, 1), jnp.float32)], axis=1)
    td_error = (
        rewards.astype(jnp.float32)
        + per_step[:, None] * jnp.where(next_valid, value_next, 0.0)
        - value_f
    )
    td_error = jnp.where(is_valid, td_error, 0.0).reshape(rows_here, blocks_here, block)
    offset = jnp.arange(block, dtype=jnp.float32)
    lower_scale = jnp.exp(-decay_rate[:, None] * offset[None, :])
    upper_scale = jnp.exp(decay_rate[:, None] * offset[None, :])
    triangle = (offset[:, None] >= offset[None, :]).astype(jnp.float32)
    scaled = td_error * lower_scale[:, None, :]
    summed = jnp.einsum("rjk,kt->rjt", scaled, triangle, precision=HIGHEST)
    local_part = summed * upper_scale[:, None, :]
    heads = local_part[:, :, 0]
    block_step = jnp.exp(-decay_rate * block)

    def carry_step(carry, head):
        fresh = head + block_step * carry
        return (fresh, fresh)

    final_carry, starts = lax.scan(carry_step, jnp.zeros_like(decay_rate), heads.T, reverse=True)
    next_heads = jnp.concatenate([starts[1:].T, jnp.zeros((rows_here, 1), jnp.float32)], axis=1)
    reach = jnp.exp(-decay_rate[:, None] * (block - offset[None, :]))
    total = local_part + reach[:, None, :] * next_heads[:, :, None]
    return jnp.where(is_valid, total.reshape(rows_here, span), 0.0).astype(jnp.bfloat16)


def by_target(array, piece_dest):
    peers = piece_dest.shape[1]
    target = piece_dest[0]
    slots = jnp.arange(peers, dtype=jnp.int32)
    source_slot = jnp.sum(jnp.where(target[None, :] == slots[:, None], slots[None, :], 0), axis=1)
    pieces = array.reshape((peers, array.shape[0] // peers) + array.shape[1:])
    return jnp.take(pieces, source_slot, axis=0).reshape(array.shape)


def reorder(received, row_perm):
    blocks_here, block = row_perm.shape
    chooser = (row_perm[:, :, None] == jnp.arange(block, dtype=jnp.int32)[None, None, :]).astype(
        jnp.bfloat16
    )

    def permute_one(member):
        shaped = member.reshape(blocks_here, block, member.shape[-1])
        mixed = jnp.einsum("bim,bmc->bic", chooser, shaped, preferred_element_type=jnp.float32)
        return mixed.astype(jnp.bfloat16).reshape(member.shape)

    return tuple((permute_one(member) for member in received))


def whiten(rewards, advantage, lengths, minibatch):
    rows_here, span = rewards.shape
    position = jnp.arange(span, dtype=jnp.int32)
    is_valid = position[None, :] < lengths[:, None]
    counted = lengths.astype(jnp.float32)
    reward_f = jnp.where(is_valid, rewards.astype(jnp.float32), 0.0)
    advantage_f = jnp.where(is_valid, advantage.astype(jnp.float32), 0.0)
    member = (minibatch[:, None] == jnp.arange(MINIBATCHES, dtype=jnp.int32)[None, :]).astype(
        jnp.float32
    )
    row_terms = jnp.stack(
        [
            counted,
            jnp.sum(reward_f, axis=1),
            jnp.sum(advantage_f, axis=1),
            jnp.sum(reward_f * reward_f, axis=1),
            jnp.sum(advantage_f * advantage_f, axis=1),
        ],
        axis=1,
    )
    totals = lax.psum(jnp.dot(member.T, row_terms, precision=HIGHEST), ("dp", "group"))
    count = jnp.maximum(totals[:, 0], 1.0)
    means = totals[:, 1:3] / count[:, None]
    spreads = totals[:, 3:5] / count[:, None] - means * means
    row_means = jnp.dot(member, means, precision=HIGHEST)
    row_scale = jnp.dot(member, lax.rsqrt(spreads + 1e-05), precision=HIGHEST)
    white_rewards = jnp.where(is_valid, (reward_f - row_means[:, 0:1]) * row_scale[:, 0:1], 0.0)
    white_advantage = jnp.where(
        is_valid, (advantage_f - row_means[:, 1:2]) * row_scale[:, 1:2], 0.0
    )
    return (white_rewards.astype(jnp.bfloat16), white_advantage.astype(jnp.bfloat16))


def plain_local(rewards, values, lengths, decay_rate, piece_dest, row_perm, minibatch):
    blocks_here, block = row_perm.shape
    new_order = (jnp.arange(blocks_here, dtype=jnp.int32)[:, None] * block + row_perm).reshape(-1)
    per_row = jnp.stack([lengths.astype(jnp.float32), decay_rate], axis=1)
    moved_terms = lax.all_to_all(
        by_target(per_row, piece_dest), "dp", split_axis=0, concat_axis=0, tiled=True
    )
    moved_terms = jnp.take(moved_terms, new_order, axis=0)
    lengths_here = moved_terms[:, 0].astype(jnp.int32)
    rate_here = moved_terms[:, 1]
    moved_rewards, moved_second = reorder(
        (
            lax.all_to_all(
                by_target(rewards, piece_dest), "dp", split_axis=0, concat_axis=0, tiled=True
            ),
            lax.all_to_all(
                by_target(values, piece_dest), "dp", split_axis=0, concat_axis=0, tiled=True
            ),
        ),
        row_perm,
    )
    advantage = discounted(moved_rewards, moved_second, lengths_here, rate_here)
    return whiten(moved_rewards, advantage, lengths_here, minibatch)


F32 = jnp.float32
BF16 = jnp.bfloat16
LANES = 128
MESH = pl.DeviceIdType.MESH
NT = (((1,), (1,)), ((), ()))


def ragged_kernel(
    n_dp, n_group, own_part, shared,
    rew_hbm, val_hbm, len_hbm, rate_hbm, dest_hbm, perm_hbm, mini_hbm,
    white_far, white_a, white_k, over_out, unused_r, unused_a,
    rbuf, vbuf, abuf, white_r, len_v, rate_v, perm_v, mini_v, dest_v,
    dsend, psend, hsend, hrecv, merged, esend, erecv, gsend, grecv, arranged, late, flag_v, dense, packed, chooser, placer, spread,
    out_st, out_ch, tri, lower, upper, lenb, bstep, carry,
    acc, tbuf, tstage, tsend, trecv, psum, precv, qsum, qrecv, tot,
    load_sem, meta_sem, own_sem, ds_sem, dr_sem, ks_sem, kr_sem, hs_sem, hr_sem, fs_sem, xs_sem, xr_sem, es_sem, er_sem, gs_sem, gr_sem,
    ts_sem, tr_sem, ps_sem, pr_sem, qs_sem, qr_sem,
):
    rows, span = rbuf.shape
    blocks = out_ch.shape[0]
    piece = rows // n_dp
    half = n_dp // 2
    chunks = span // LANES
    quarter = half // 2
    depth = own_part + shared
    wide = tri.shape[0]
    cuts = part_cuts(own_part)
    me = lax.axis_index("dp")
    mine = lax.axis_index("group")
    side = me // half
    spot = lax.rem(me, half)
    column = lax.rem(spot, quarter)
    level = spot // quarter

    def dp_peer(d):
        return lax.rem(me + d, n_dp)

    def group_peer(d):
        return lax.rem(mine + d, n_group)

    def near(j):
        return side * half + lax.rem(me + j, half)

    def across(i, f):
        goal = lax.rem(level + f, 2)
        return (1 - side) * half + goal * quarter + lax.rem(column + i, quarter)

    small = []
    for i, (src, dst) in enumerate(
        ((len_hbm, len_v), (dest_hbm, dest_v), (rate_hbm, rate_v), (perm_hbm, perm_v), (mini_hbm, mini_v))
    ):
        small.append(pltpu.make_async_copy(src, dst, meta_sem.at[i]))
        small[-1].start()
    step = rows // 4
    loads = []
    for x, (src, dst) in enumerate(((rew_hbm, rbuf), (val_hbm, vbuf))):
        for part in range(4):
            at = pl.ds(part * step, step)
            loads.append(pltpu.make_async_copy(src.at[at], dst.at[at], load_sem.at[x, part]))
            loads[-1].start()

    barrier = pltpu.get_barrier_semaphore()
    for d in range(1, n_dp):
        pl.semaphore_signal(barrier, inc=1, device_id=(dp_peer(d), mine), device_id_type=MESH)
    for d in range(1, n_group):
        pl.semaphore_signal(barrier, inc=1, device_id=(me, group_peer(d)), device_id_type=MESH)

    lane = lax.broadcasted_iota(jnp.int32, (LANES, LANES), 1)
    sub = lax.broadcasted_iota(jnp.int32, (LANES, LANES), 0)
    before = jnp.logical_and(sub // piece == lane // piece, sub < lane).astype(F32).astype(BF16)
    per_vreg = LANES // piece

    def used(length):
        return ((length + (LANES - 1)) // LANES).astype(F32).astype(BF16)

    for copy in small:
        copy.wait()

    dests = [dest_v[0:1, p : p + 1] for p in range(n_dp)]
    targets = [jnp.broadcast_to(dest.astype(F32), (piece, LANES)) for dest in dests]
    row_dest = []
    for b in range(blocks):
        here = jnp.zeros((16, LANES), jnp.int32)
        for q in range(per_vreg):
            here = jnp.where(lane[0:16] // piece == q, dests[b * per_vreg + q], here)
        row_dest.append(here)
    fold = (sub % piece == lane % piece).astype(F32).astype(BF16)

    def pick(k, source):
        k = jnp.full((piece, LANES), k, jnp.int32).astype(F32)
        weights = [(target == k).astype(F32).astype(source.dtype) for target in targets]
        for c in range(0, source.shape[1], LANES):
            at = slice(c, c + LANES)
            yield at, sum(source[p * piece : (p + 1) * piece, at] * weights[p] for p in range(n_dp))

    counts = {}

    def choose(i, f):
        wanted = jnp.zeros((16, LANES), F32)
        for b in range(blocks):
            here = jnp.broadcast_to(len_v[b : b + 1, :], (16, LANES))
            here = jnp.where(row_dest[b] == across(i, f), here, 0)
            wanted = wanted + jnp.dot(used(here), fold, preferred_element_type=F32)
        base = jnp.dot(wanted.astype(BF16), before, preferred_element_type=F32)
        taken = jnp.max((base + wanted)[0:8], axis=1, keepdims=True)
        base = base.astype(jnp.int32)[0:1]
        wanted = wanted.astype(jnp.int32)[0:1]
        counts[i, f] = base, wanted
        match_rows(chooser, i, f, own_part, base, wanted)
        esend[2 * i + f] = jnp.maximum(jnp.broadcast_to(taken, (8, LANES)) - own_part, 0.0)

    def match_rows(target, i, f, size, base, wanted):
        place = lax.broadcasted_iota(jnp.int32, (size, LANES), 0)
        for v in range(chunks // per_vreg):
            c = lane[0:1] // piece + v * per_vreg
            key = jnp.where(c < wanted, base + c, -1)
            at = slice(v * LANES, (v + 1) * LANES)
            target[i, f, :, at] = (place == key).astype(F32).astype(BF16)

    def pack(x, i, f, source):
        for c, (_, part) in enumerate(pick(across(i, f), source)):
            arranged[x, i, f, c * piece : (c + 1) * piece, :] = part
        psend[x, i, f] = jnp.dot(
            chooser[i, f], arranged[x, i, f], preferred_element_type=F32
        ).astype(BF16)

    def ahead(table, own):
        total = jnp.zeros_like(own)
        for m in range(n_group):
            total = total + jnp.where(jnp.full(own.shape, m, jnp.int32) < mine, table[m], 0.0)
        return total

    def pack_late():
        for i in range(quarter):
            for f in range(2 if shared else 0):
                base, wanted = counts[i, f]
                skip = ahead(erecv[:, 2 * i + f], esend[2 * i + f])[0:1].astype(jnp.int32)
                base = base + skip - own_part
                c = lane[0:1] // piece
                place = lax.broadcasted_iota(jnp.int32, (shared, LANES), 0)
                for v in range(chunks // per_vreg):
                    c = lane[0:1] // piece + v * per_vreg
                    key = jnp.where(jnp.logical_and(c < wanted, base + c >= skip), base + c, -1)
                    at = slice(v * LANES, (v + 1) * LANES)
                    late[:, at] = (place == key).astype(F32).astype(BF16)
                for x in range(2):
                    hsend[x, 2 * i + f] = jnp.dot(
                        late[...], arranged[x, i, f], preferred_element_type=F32
                    ).astype(BF16)

    def copy_dense(x, j, source):
        for at, part in pick(near(j), source):
            dsend[x, j, :, at] = part

    for load in loads[:4]:
        load.wait()

    def remote(src, dst, send, recv, who):
        return pltpu.make_async_remote_copy(
            src_ref=src, dst_ref=dst, send_sem=send, recv_sem=recv,
            device_id=who, device_id_type=MESH,
        )

    def dense_copy(x, j):
        return remote(
            dsend.at[x, j], dense.at[x, spot], ds_sem.at[x, j], dr_sem.at[x, j], (near(j), mine)
        )

    def packed_copy(x, i, f, part):
        at = pl.ds(*cuts[x][part])
        return remote(
            psend.at[x, i, f, at], packed.at[x, spot, at],
            ks_sem.at[x, part, i, f], kr_sem.at[x, part, spot], (across(i, f), mine),
        )

    last = pl.ds(own_part, shared)

    others = range(1, n_group if shared else 1)

    def swap_copy(x, d):
        k = group_peer(d)
        return remote(
            hsend.at[x, k], hrecv.at[x, mine], xs_sem.at[x, d], xr_sem.at[x, d], (me, k)
        )

    def shared_copy(x):
        return remote(
            merged.at[x], packed.at[x, spot, last],
            hs_sem.at[x], hr_sem.at[x, spot], (across(mine // 2, lax.rem(mine, 2)), mine),
        )

    def held_by(m):
        return lax.rem(level + lax.rem(m, 2), 2) * quarter + lax.rem(column + m // 2, 2)

    def relay_copy(x, m, d):
        q = held_by(m)
        return remote(
            packed.at[x, q, last], packed.at[x, q, last],
            fs_sem.at[x, d], hr_sem.at[x, q], (me, group_peer(d)),
        )

    def swap(x):
        for d in others:
            swap_copy(x, d).start()

    def merge(x):
        if shared:
            total = hsend[x, mine]
            for d in others:
                swap_copy(x, d).wait_recv()
            for d in others:
                total = total + hrecv[x, group_peer(d)]
            merged[x] = total

    def send_merged(x):
        if shared:
            shared_copy(x).start()

    def receive_packed(x, part):
        at = pl.ds(*cuts[x][part])
        for q in range(half):
            remote(
                psend.at[x, 0, 0, at], packed.at[x, q, at],
                ks_sem.at[x, part, 0, 0], kr_sem.at[x, part, q], (across(0, 0), mine),
            ).wait_recv()

    def relay(x):
        if shared:
            relay_copy(x, mine, 1).wait_recv()
        for d in others:
            relay_copy(x, mine, d).start()

    def relayed(x):
        for d in others:
            relay_copy(x, group_peer(d), 1).wait_recv()

    order = []
    for i in range(quarter):
        for f in range(2):
            order.append(("own", i, f))
            if len(order) < n_dp - 1:
                order.append(("near", i * 2 + f + 1, 0))

    def stage(item):
        kind, i, f = item
        if kind == "near":
            copy_dense(0, i, rbuf)
        else:
            choose(i, f)
            pack(0, i, f, rbuf)

    sent = []

    def issue(x, item):
        kind, i, f = item
        if kind == "near":
            dense_sent[x].append(dense_copy(x, i))
            dense_sent[x][-1].start()
        else:
            sent.append(packed_copy(x, i, f, 0))
            sent[-1].start()

    dense_sent = [[], []]
    stage(order[0])
    pl.semaphore_wait(barrier, n_dp + n_group - 2)
    held = len(order) - 2
    for item, later in zip(order[:held], order[1:]):
        stage(later)
        issue(0, item)

    for b in range(blocks):
        at = pl.ds(b * LANES, LANES)
        rate = jnp.transpose(jnp.broadcast_to(rate_v[b : b + 1, :], (LANES, LANES)))
        length = jnp.transpose(jnp.broadcast_to(len_v[b : b + 1, :].astype(F32), (LANES, LANES)))
        lenb[at, :] = length.astype(jnp.int32)
        bstep[at, :] = jnp.exp(-rate * wide)
        carry[at, :] = jnp.zeros((LANES, LANES), F32)
        for x in range(4):
            acc[x, at, :] = jnp.zeros((LANES, LANES), F32)
        for i in range(wide // LANES):
            offset = (lane + i * LANES).astype(F32)
            lower[at, i * LANES : (i + 1) * LANES] = jnp.exp(-rate * offset)
            upper[at, i * LANES : (i + 1) * LANES] = jnp.exp(rate * offset)
    tri[...] = (
        lax.broadcasted_iota(jnp.int32, (wide, wide), 0)
        >= lax.broadcasted_iota(jnp.int32, (wide, wide), 1)
    ).astype(F32).astype(BF16)
    for load in loads[4:]:
        load.wait()

    reps = wide // LANES

    def column_step(i, _):
        col = pl.multiple_of((span // wide - 1 - i) * wide, wide)
        for b in range(blocks):
            at = pl.ds(b * LANES, LANES)
            length = lenb[at, :]
            position = col + lax.broadcasted_iota(jnp.int32, (LANES, wide), 1)
            valid = position < jnp.concatenate([length] * reps, axis=1)
            r = jnp.where(valid, rbuf[at, pl.ds(col, wide)].astype(F32), 0.0)
            s = r * lower[at, :]
            high = s.astype(BF16)
            low = (s - high.astype(F32)).astype(BF16)
            both = jnp.dot(
                jnp.concatenate([high, low], axis=0), tri[...], preferred_element_type=F32
            )
            c = carry[at, :]
            summed = both[:LANES] + both[LANES:] + jnp.concatenate([c] * reps, axis=1)
            carry[at, :] = bstep[at, :] * jnp.broadcast_to(summed[:, :1], (LANES, LANES))
            a = upper[at, :] * summed - vbuf[at, pl.ds(col, wide)].astype(F32)
            a = jnp.where(valid, a, 0.0).astype(BF16)
            abuf[at, pl.ds(col, wide)] = a
            a = a.astype(F32)
            for x, term in enumerate((r, a, r * r, a * a)):
                acc[x, at, :] += sum(term[:, i * LANES : (i + 1) * LANES] for i in range(reps))
        return 0

    lax.fori_loop(0, span // wide, column_step, 0)

    for b in range(blocks):
        at = pl.ds(b * LANES, LANES)
        terms = jnp.where(lane == 0, lenb[at, :].astype(F32), 0.0)
        for x in range(4):
            total = jnp.sum(acc[x, at, :], axis=1, keepdims=True)
            terms = jnp.where(lane == x + 1, total, terms)
        tbuf[at, :] = terms
    tstage[...] = jnp.zeros_like(tstage)

    def stage_terms(d, _):
        for at, part in pick(dp_peer(d), tbuf):
            tstage[0:piece, :] = part
        tsend[d] = jnp.transpose(tstage[...])[0:8, :]
        return 0

    lax.fori_loop(0, n_dp, stage_terms, 0)

    terms_sent = []
    for d in range(1, n_dp):
        k = dp_peer(d)
        terms_sent.append(remote(tsend.at[d], trecv.at[me], ts_sem.at[d], tr_sem.at[d], (k, mine)))
        terms_sent[-1].start()
    trecv[me] = tsend[0]
    for item, later in zip(order[held:], order[held + 1 :] + [("near", 0, 0)]):
        stage(later)
        issue(0, item)
    own = [pltpu.make_async_copy(dsend.at[0, 0], dense.at[0, spot], own_sem.at[0])]
    own[0].start()
    tells = []
    for d in range(1, n_group):
        k = group_peer(d)
        tells.append(remote(esend, erecv.at[mine], es_sem.at[d], er_sem.at[d], (me, k)))
        tells[-1].start()
    erecv[mine] = esend[...]
    for i in range(quarter):
        for f in range(2):
            pack(1, i, f, abuf)
    for j in range(half):
        copy_dense(1, j, abuf)
    for copy in tells:
        copy.wait()
    pack_late()
    swap(0)
    swap(1)

    for copy in terms_sent:
        copy.wait()
    other = 1 - side
    length = trecv[other * (LANES // piece)]
    for q in range(1, LANES // piece):
        length = length + pltpu.roll(trecv[other * (LANES // piece) + q], q * piece, 1)
    length = jnp.broadcast_to(length[0:1], (16, LANES)).astype(jnp.int32)
    wanted = used(length)
    base = jnp.dot(wanted, before, preferred_element_type=F32)
    alike = (sub // piece == lane // piece).astype(F32).astype(BF16)
    beyond = jnp.dot(wanted, alike, preferred_element_type=F32)[0:8] - own_part
    gsend[...] = jnp.maximum(beyond, 0.0)
    grecv[mine] = gsend[...]
    for d in range(1, n_group):
        k = group_peer(d)
        tells.append(remote(gsend, grecv.at[mine], gs_sem.at[d], gr_sem.at[d], (me, k)))
        tells[-1].start()

    row = sub.astype(F32)
    over = jnp.zeros((8, LANES), F32)
    for slot in range(half):
        filled = erecv[0, slot]
        for m in range(1, n_group):
            filled = filled + erecv[m, slot]
        over = jnp.where(filled > shared, 1.0, over)
    partial = jnp.where(lax.broadcasted_iota(jnp.int32, (8, LANES), 0) == 5, over, 0.0)
    per_block = LANES // piece
    for b in range(blocks):
        picked = (row == perm_v[b : b + 1, :].astype(F32)).astype(F32)
        member = (row == mini_v[b : b + 1, :].astype(F32)).astype(F32)
        arrived_member = lax.dot_general(
            member.astype(BF16), picked.astype(BF16), NT, preferred_element_type=F32
        )
        terms = trecv[b * per_block]
        for s in range(1, per_block):
            terms = terms + pltpu.roll(trecv[b * per_block + s], s * piece, 1)
        partial = partial + lax.dot_general(
            terms, arrived_member, NT, precision=HIGHEST, preferred_element_type=F32
        )
        out_ch[b] = jnp.transpose(picked).astype(BF16)
        tot[b] = jnp.dot(terms, picked, precision=HIGHEST, preferred_element_type=F32)
    psum[...] = partial
    precv[me] = partial
    sums_sent = []
    for d in range(1, n_dp):
        k = dp_peer(d)
        sums_sent.append(remote(psum, precv.at[me], ps_sem.at[d], pr_sem.at[d], (k, mine)))
        sums_sent[-1].start()

    for x in range(2):
        merge(x)
    send_merged(0)
    send_merged(1)
    for item in order:
        issue(1, item)
    own.append(pltpu.make_async_copy(dsend.at[1, 0], dense.at[1, spot], own_sem.at[1]))
    own[1].start()
    for part in range(1, len(cuts[1])):
        for i in range(quarter):
            for f in range(2):
                sent.append(packed_copy(1, i, f, part))
                sent[-1].start()

    for copy in tells[n_group - 1 :]:
        copy.wait()
    skip = ahead(grecv, gsend[...])
    skip = jnp.transpose(jnp.broadcast_to(skip[0:1], (LANES, LANES))).astype(jnp.int32)
    base = jnp.transpose(jnp.broadcast_to(base[0:1], (LANES, LANES))).astype(jnp.int32)
    wanted = jnp.transpose(jnp.broadcast_to(wanted.astype(F32)[0:1], (LANES, LANES))).astype(jnp.int32)

    def place_chunk(c, _):
        key = base + c
        key = jnp.where(key >= own_part, key + skip, key)
        key = jnp.where(c < wanted, key, -1)
        at = pl.ds(pl.multiple_of(c * piece, piece), piece)
        for n in range(depth // LANES):
            match = (lane + n * LANES == key).astype(F32).astype(BF16)
            for q in range(half):
                placer[q, at, n * LANES : (n + 1) * LANES] = match[q * piece : (q + 1) * piece]
        return 0

    lax.fori_loop(0, chunks, place_chunk, 0)

    def unpack(x, start, stop, first):
        stop = depth if stop == own_part else stop

        def one(q, _):
            got = jnp.dot(
                placer[q, :, start:stop], packed[x, q, start:stop, :], preferred_element_type=F32
            ).astype(BF16)
            at = pl.ds(pl.multiple_of(q * piece, piece), piece)
            for c in range(chunks):
                cols = slice(c * LANES, (c + 1) * LANES)
                part = got[c * piece : (c + 1) * piece]
                spread[x, at, cols] = part if first else spread[x, at, cols] + part
            return 0

        lax.fori_loop(0, half, one, 0, unroll=2)

    for copy in own[:1] + dense_sent[0]:
        copy.wait()
    relay(0)
    receive_packed(0, 0)
    relayed(0)
    unpack(0, 0, own_part, True)
    relay(1)

    for copy in sums_sent:
        copy.wait()
    partial = precv[0]
    for k in range(1, n_dp):
        partial = partial + precv[k]
    qsum[...] = partial
    qrecv[mine] = partial
    group_sent = []
    for d in range(1, n_group):
        k = group_peer(d)
        group_sent.append(remote(qsum, qrecv.at[mine], qs_sem.at[d], qr_sem.at[d], (me, k)))
        group_sent[-1].start()
    for copy in group_sent:
        copy.wait()
    total = qrecv[0]
    for k in range(1, n_group):
        total = total + qrecv[k]
    flag_v[...] = jnp.full((8, LANES), jnp.max(total[5:6, :]))
    flag_copy = pltpu.make_async_copy(flag_v, over_out, own_sem.at[3])
    flag_copy.start()

    count = jnp.maximum(total[0:1, :], 1.0)
    means = total[1:3, :] / count
    spreads = jnp.maximum(total[3:5, :] / count - means * means, 0.0)
    scales = lax.rsqrt(spreads + 1e-05)
    table = jnp.concatenate([means, scales, jnp.zeros((4, LANES), F32)], axis=0)
    for b in range(blocks):
        at = pl.ds(b * LANES, LANES)
        member = (row == mini_v[b : b + 1, :].astype(F32)).astype(F32)
        here = jnp.dot(table, member, precision=HIGHEST, preferred_element_type=F32)
        here = jnp.concatenate(
            [here[0:4, :], tot[b, 0:1, :], jnp.zeros((LANES - 5, LANES), F32)], axis=0
        )
        out_st[at, :] = jnp.transpose(here)

    def whiten_block(x, arrived_at, b, target):
        tile = 1024

        def tile_step(i, _):
            col = pl.multiple_of(i * tile, tile)
            at = pl.ds(pl.multiple_of(b * LANES, LANES), LANES)
            stats = out_st[at, :]
            position = (col + lax.broadcasted_iota(jnp.int32, (LANES, tile), 1)).astype(F32)
            moved = jnp.dot(out_ch[b], arrived_at(pl.ds(col, tile)), preferred_element_type=F32)
            white = (moved - stats[:, x : x + 1]) * stats[:, x + 2 : x + 3]
            white = jnp.where(position < stats[:, 4:5], white, 0.0)
            target[at, pl.ds(col, tile)] = white.astype(BF16)
            return 0

        lax.fori_loop(0, span // tile, tile_step, 0, unroll=2)

    def whiten_dense(x, target):
        whiten_block(x, lambda at: dense[x, :, :, at].reshape(LANES, at.size), side, target)

    def whiten_packed(x, target):
        whiten_block(x, lambda at: spread[x, :, at], other, target)

    whiten_dense(0, white_r)
    whiten_packed(0, white_r)
    rest = rows - white_k.shape[0]
    kept = pltpu.make_async_copy(
        white_r.at[pl.ds(0, rest)], white_far.at[pl.ds(0, rest)], own_sem.at[2]
    )
    kept.start()
    white_k[...] = white_r[rest:, :]
    for copy in own[1:] + dense_sent[1]:
        copy.wait()
    whiten_dense(1, white_a)
    for part, (start, size) in enumerate(cuts[1]):
        receive_packed(1, part)
        if part == len(cuts[1]) - 1:
            relayed(1)
        unpack(1, start, start + size, part == 0)
    whiten_packed(1, white_a)
    for copy in sent:
        copy.wait_send()
    for x in range(2 if shared else 0):
        shared_copy(x).wait_send()
        for d in others:
            swap_copy(x, d).wait_send()
            relay_copy(x, mine, d).wait_send()
    kept.wait()
    flag_copy.wait()


def part_cuts(size):
    b = (size - 1) // 128 * 128
    return (((0, size),), ((0, b), (b, size - b)))


def ragged(n_dp, n_group, own_part, shared, collective_id, spare, rewards, values, lengths, decay_rate, piece_dest, row_perm, minibatch):
    rows, span = rewards.shape
    blocks, block = row_perm.shape
    piece = rows // n_dp
    half = n_dp // 2
    wide = 256
    depth = own_part + shared
    extra = max(shared, 16)
    chunks = piece * (span // LANES)
    vmem = pl.BlockSpec(memory_space=pltpu.VMEM)
    far = pl.BlockSpec(memory_space=pltpu.HBM)
    dma = pltpu.SemaphoreType.DMA
    whole = pltpu.VMEM((rows, span), BF16)
    factor = pltpu.VMEM((rows, wide), F32)
    column = pltpu.VMEM((rows, LANES), F32)
    small = pltpu.VMEM((n_dp, 8, LANES), F32)
    one = pltpu.VMEM((8, LANES), F32)
    meta = pltpu.VMEM((blocks, LANES), jnp.int32)
    dense = pltpu.VMEM((2, half, piece, span), BF16)
    parts = len(part_cuts(own_part)[1])
    return pl.pallas_call(
        functools.partial(ragged_kernel, n_dp, n_group, own_part, shared),
        out_shape=tuple(
            jax.ShapeDtypeStruct((k, span), BF16) for k in (spare * rows, rows, rows * 5 // 8)
        )
        + (jax.ShapeDtypeStruct((8, LANES), F32),)
        + (jax.ShapeDtypeStruct((rows, span), BF16),) * 2,
        in_specs=[far] * 7,
        out_specs=(far, vmem, vmem, far, far, far),
        scratch_shapes=[
            whole, whole, whole, whole, meta, pltpu.VMEM((blocks, LANES), F32), meta, meta,
            pltpu.VMEM((1, n_dp), jnp.int32),
            dense, pltpu.VMEM((2, half // 2, 2, own_part, LANES), BF16),
            pltpu.VMEM((2, half, extra, LANES), BF16), pltpu.VMEM((2, n_group, extra, LANES), BF16),
            pltpu.VMEM((2, extra, LANES), BF16),
            pltpu.VMEM((half, 8, LANES), F32), pltpu.VMEM((n_group, half, 8, LANES), F32),
            one, pltpu.VMEM((n_group, 8, LANES), F32),
            pltpu.VMEM((2, 2, 2, chunks, LANES), BF16), pltpu.VMEM((extra, chunks), BF16), one,
            dense, pltpu.VMEM((2, half, depth, LANES), BF16),
            pltpu.VMEM((half // 2, 2, own_part, chunks), BF16), pltpu.VMEM((half, chunks, depth), BF16),
            pltpu.VMEM((2, LANES, span), BF16),
            column, pltpu.VMEM((blocks, LANES, LANES), BF16),
            pltpu.VMEM((wide, wide), BF16), factor, factor,
            pltpu.VMEM((rows, LANES), jnp.int32), column, column,
            pltpu.VMEM((4, rows, LANES), F32), column, pltpu.VMEM((LANES, LANES), F32),
            small, small, one, small, one, pltpu.VMEM((n_group, 8, LANES), F32),
            pltpu.VMEM((blocks, 8, LANES), F32),
            dma((2, 4)), dma((5,)), dma((4,)), dma((2, half)), dma((2, half)),
            dma((2, parts, half // 2, 2)), dma((2, parts, half)),
            dma((2,)), dma((2, half)), dma((2, n_group)), dma((2, n_group)), dma((2, n_group)),
            dma((n_group,)), dma((n_group,)), dma((n_group,)), dma((n_group,)),
            dma((n_dp,)), dma((n_dp,)), dma((n_dp,)), dma((n_dp,)), dma((n_group,)), dma((n_group,)),
        ],
        compiler_params=pltpu.CompilerParams(
            collective_id=collective_id, has_side_effects=True, vmem_limit_bytes=52_000_000
        ),
    )(
        rewards, values, lengths.reshape(blocks, block), decay_rate.reshape(blocks, block),
        piece_dest, row_perm, minibatch.reshape(blocks, block),
    )


def write_kernel(
    over_far, from_r, from_a, from_k, whole_r, whole_a, to_r, to_a, bounce, over, sem
):
    rows, kept = from_a.shape[0], from_k.shape[0]
    rest = rows - kept

    def started(src, dst, at):
        copy = pltpu.make_async_copy(src, dst, sem.at[at])
        copy.start()
        return copy

    flag = started(over_far, over, 0)
    half = rest // 2
    parts = [pl.ds(half * k, half) for k in range(2)]
    reads = [started(from_r.at[at], bounce.at[at], 1 + k) for k, at in enumerate(parts)]
    writes = []
    for k in range(2):
        at = pl.ds(k * rows // 2, rows // 2)
        writes.append(started(from_a.at[at], to_a.at[at], 3 + k))
    writes.append(started(from_k, to_r.at[pl.ds(rest, kept)], 5))
    for k, at in enumerate(parts):
        reads[k].wait()
        writes.append(started(bounce.at[at], to_r.at[at], 6 + k))
    flag.wait()
    for copy in writes:
        copy.wait()

    @pl.when(jnp.max(over[...]) > 0.0)
    def _():
        for source, target in ((whole_r, to_r), (whole_a, to_a)):
            started(source, bounce, 1).wait()
            started(bounce, target, 1).wait()


def write(over, results, whole_way):
    vmem = pl.BlockSpec(memory_space=pltpu.VMEM)
    far = pl.BlockSpec(memory_space=pltpu.HBM)
    shape = whole_way[0].shape
    return tuple(
        pl.pallas_call(
            write_kernel,
            out_shape=[jax.ShapeDtypeStruct(x.shape, x.dtype) for x in whole_way],
            in_specs=[far, far, vmem, vmem, far, far],
            out_specs=[far, far],
            scratch_shapes=[
                pltpu.VMEM(shape, BF16), pltpu.VMEM(over.shape, F32), pltpu.SemaphoreType.DMA((8,)),
            ],
            compiler_params=pltpu.CompilerParams(vmem_limit_bytes=52_000_000),
        )(over, *results, *whole_way)
    )


def local(n_dp, n_group, rewards, values, lengths, decay_rate, piece_dest, row_perm, minibatch):
    rows, span = rewards.shape
    blocks, block = row_perm.shape
    piece = rows // n_dp
    args = (rewards, values, lengths, decay_rate, piece_dest, row_perm, minibatch)
    if piece % 16 or LANES % piece or block != LANES or span % 4096:
        return plain_local(*args)
    if n_dp // 4 != 2 or n_dp % 4 or n_group != 4 or blocks != 2 or n_dp // 2 * piece != LANES:
        return plain_local(*args)
    chunks = piece * (span // LANES)
    own_part, shared = chunks * 36 // 64, chunks * 12 // 64

    def whole(results):
        kept = results[2]
        rest = rows - kept.shape[0]
        return jnp.concatenate([results[0][:rest], kept], axis=0), results[1]

    *results, over, unused_r, unused_a = ragged(
        n_dp, n_group, own_part, shared, 0, 8, *args
    )
    whole_way = lax.cond(
        over[0, 0] > 0.0,
        lambda unused, args: whole(ragged(n_dp, n_group, chunks, 0, 1, 1, *args)),
        lambda unused, args: tuple(unused),
        (unused_r, unused_a), args,
    )
    return write(over, results, whole_way)


def solution(mesh):
    return jax.shard_map(
        functools.partial(local, mesh.shape["dp"], mesh.shape["group"]),
        mesh=mesh,
        in_specs=(
            P(("dp", "group"), None),
            P(("dp", "group"), None),
            P(("dp", "group")),
            P(("dp", "group")),
            P("dp", None),
            P(("dp", "group"), None),
            P(("dp", "group")),
        ),
        out_specs=(P(("dp", "group"), None), P(("dp", "group"), None)),
        check_vma=False,
    )
```
